256 devices in a mesh: ep: 32 (over x, z), tp: 8 (over y, core).
Axes of the slice: x: 4, y: 4, z: 8, core: 2. Of those that a mesh axis runs over, the one named last changes fastest.
Arguments:
- tokens: bfloat16 [4096, 3072], P('ep', 'tp'), may hold values from -6 to 6
- expert_ids: int32 [4096, 2], P('ep'), may hold values from 0 to 7, all different within a row
- route_share: float32 [4096], P('ep'), may hold values from 0.5 to 0.95
- w_gate: bfloat16 [65536, 3072], P(('ep', 'tp')), may hold values from -0.109375 to 0.109375
- w_up: bfloat16 [65536, 3072], P(('ep', 'tp')), may hold values from -0.109375 to 0.109375
- w_down: bfloat16 [65536, 3072], P(('ep', 'tp')), may hold values from -0.0625 to 0.0625
- reward_head: float32 [3072], P('tp'), may hold values from -0.109375 to 0.109375
- upstream: bfloat16 [4096, 3072], P('ep', 'tp'), may hold values from -4 to 4
- pair_order: int32 [64], replicated, may hold values from 0 to 63, each once
Outputs:
- layer_out: bfloat16 [4096, 3072], P('ep', 'tp')
- rewards: float32 [64], replicated
- pair_loss: float32 [], replicated
- grad_tokens: bfloat16 [4096, 3072], P('ep', 'tp')
- grad_gate: bfloat16 [65536, 3072], P(('ep', 'tp'))
- grad_up: bfloat16 [65536, 3072], P(('ep', 'tp'))
- grad_down: bfloat16 [65536, 3072], P(('ep', 'tp'))
The draws below stay inside these ranges and needn't reach their ends.
Inputs may be any that keep to these rules, and one draw needn't show every extreme that they name: `expert_ids`: each row names 2 different experts. `pair_order`: each of the 64 sequence indices appears once.
All inputs are finite; a program needn't handle non-finite values.
Results may differ from the reference program's by a relative error of at most 0.014.
Values may be sent and summed in bfloat16 or wider, within the bound.
No kernel may reach another device: no remote copies, remote signals or barrier semaphores. Data moves between devices by JAX's collectives and lax.ppermute only.
A program may use at most 128 MiB of HBM per device.

```python
import math
from functools import partial
import jax
import jax.numpy as jnp
from jax import lax

D = 3072
FF = 8192
EXPERTS = 8
TOPK = 2
SEQ_LEN = 64
TOK_DEV = 128
TOKENS = 4096
SEQS = 64
N_EP = 32
N_TP = 8


def shard_levels(own_key, extent, shards, smallest, high):
    factor_of = 1.0
    for axis_at, blocks in shards:
        draws = jax.random.uniform(jax.random.fold_in(jax.random.fold_in(own_key, 6), axis_at), (blocks,), jnp.float32, smallest / len(shards), high / len(shards))
        factor_of = factor_of * jnp.repeat(jnp.exp(draws), extent[axis_at] // blocks).reshape((-1,) + (1,) * (len(extent) - 1 - axis_at))
    return factor_of


def choose_distinct(own_key, rows, count, top, lift):
    sequence = jax.random.permutation(jax.random.fold_in(own_key, 1), count)
    favour = sequence
    for power in range(3):
        favour = favour * favour // count
    favour = favour * lift // count
    lots = jax.random.randint(jax.random.fold_in(own_key, 2), (rows, count), 0, 4096) + favour
    fixed_rows = jax.random.permutation(jax.random.fold_in(own_key, 3), rows)[jnp.arange(count) % rows]
    lots = jnp.where(jnp.arange(rows)[:, None] == fixed_rows[None, :], 1 << 14, lots)
    score = lots * count + jnp.arange(count)
    return lax.top_k(score.astype(jnp.int32), top)[1].astype(jnp.int32)


def centred(rng, extent, deviation, most, split=(), kind=jnp.bfloat16):
    gain = shard_levels(rng, extent, split, -0.22, 0.18) if split else 1.0
    entries = jax.random.normal(rng, extent, jnp.float32) * deviation * gain
    return jnp.minimum(jnp.maximum(entries, -most), most).astype(kind)


def setup_inputs(seed: int = 0) -> dict:
    seeds = jax.random.split(jax.random.key(seed), 10)
    return {
        "tokens": centred(seeds[0], (TOKENS, D), 1.0, 6.0, ((0, 32), (1, 8))),
        "expert_ids": choose_distinct(seeds[1], TOKENS, EXPERTS, TOPK, 2048),
        "route_share": jnp.clip(0.5 + 0.45 * jax.random.uniform(seeds[2], (TOKENS,), jnp.float32) ** shard_levels(seeds[2], (TOKENS,), ((0, 32),), -0.2, 0.2), 0.5, 0.95),
        "w_gate": centred(seeds[3], (EXPERTS * FF, D), D ** -0.5, 0.109375, ((0, 256),)),
        "w_up": centred(seeds[4], (EXPERTS * FF, D), D ** -0.5, 0.109375, ((0, 256),)),
        "w_down": centred(seeds[5], (EXPERTS * FF, D), FF ** -0.5, 0.0625, ((0, 256),)),
        "reward_head": centred(seeds[6], (D,), D ** -0.5, 0.109375, ((0, 8),), jnp.float32),
        "upstream": centred(seeds[7], (TOKENS, D), 0.5, 4.0, ((0, 32), (1, 8))),
        "pair_order": jax.random.permutation(seeds[8], SEQS).astype(jnp.int32),
    }


loss_scale = 256.0
highest = lax.Precision.HIGHEST

def route_tables(expert_ids, route_share, capacity):
    experts_iota = jnp.arange(EXPERTS, dtype=jnp.int32)
    first_hot = (expert_ids[:, 0:1] == experts_iota[None, :]).astype(jnp.int32)
    second_hot = (expert_ids[:, 1:2] == experts_iota[None, :]).astype(jnp.int32)
    first_rank = lax.optimization_barrier(jnp.sum((jnp.cumsum(first_hot, axis=0) - first_hot) * first_hot, axis=1))
    second_before = jnp.cumsum(second_hot, axis=0) - second_hot + lax.optimization_barrier(jnp.sum(first_hot, axis=0))[None, :]
    second_rank = lax.optimization_barrier(jnp.sum(second_before * second_hot, axis=1))
    route_ranks = jnp.stack([first_rank, second_rank], axis=1).astype(jnp.int32)
    route_kept = route_ranks < capacity
    slot_index = jnp.where(route_kept, expert_ids * capacity + route_ranks, -1).astype(jnp.int32)
    shares = jnp.stack([route_share, 1.0 - route_share], axis=1) * route_kept.astype(jnp.float32)
    slot_iota = jnp.arange(EXPERTS * capacity, dtype=jnp.int32)
    matches = (slot_index[:, :, None] == slot_iota[None, None, :]).astype(jnp.float32)
    picker = lax.optimization_barrier(jnp.sum(matches, axis=1))
    mixing = lax.optimization_barrier(jnp.sum(matches * shares[:, :, None], axis=1))
    return (picker, mixing)

def silu_parts(gate_pre):
    sigmoid_value = jax.nn.sigmoid(gate_pre)
    return (gate_pre * sigmoid_value, sigmoid_value * (1.0 + gate_pre * (1.0 - sigmoid_value)))

def block_sum(lefts, rights):
    group_size = FF // (N_EP // EXPERTS * N_TP)
    group_count = FF // group_size
    row_count = lefts[0].shape[0]
    col_count = rights[0].shape[1]
    left_blocks = tuple((matrix.reshape(row_count, group_count, group_size).transpose(1, 0, 2) for matrix in lefts))
    right_blocks = tuple((matrix.reshape(group_count, group_size, col_count) for matrix in rights))

    def accumulate(running, pieces):
        left_set, right_set = pieces
        partial_sum = jnp.dot(left_set[0], right_set[0], preferred_element_type=jnp.float32)
        for position in range(1, len(left_set)):
            partial_sum = partial_sum + jnp.dot(left_set[position], right_set[position], preferred_element_type=jnp.float32)
        rounded = lax.optimization_barrier(partial_sum.astype(jnp.bfloat16))
        return (running + rounded.astype(jnp.float32), None)
    start_value = jnp.zeros((row_count, col_count), jnp.float32)
    return lax.scan(accumulate, start_value, (left_blocks, right_blocks))[0]

def project(rows_in, weight):
    return lax.dot_general(rows_in, weight, (((1,), (1,)), ((), ())), preferred_element_type=jnp.float32)

def expert_forward(operands):
    rows_in, gate_w, up_w, down_w = operands
    gate_pre = project(rows_in, gate_w)
    up_pre = project(rows_in, up_w)
    silu_value, silu_slope = silu_parts(gate_pre)
    hidden = (silu_value * up_pre).astype(jnp.bfloat16)
    return block_sum((hidden,), (down_w,))

def expert_backward(operands):
    rows_in, grads_in, gate_w, up_w, down_w = operands
    gate_pre = project(rows_in, gate_w)
    up_pre = project(rows_in, up_w)
    silu_value, silu_slope = silu_parts(gate_pre)
    hidden = (silu_value * up_pre).astype(jnp.bfloat16)
    hidden_grad = project(grads_in, down_w)
    gate_grad = (hidden_grad * up_pre * silu_slope).astype(jnp.bfloat16)
    up_grad = (hidden_grad * silu_value).astype(jnp.bfloat16)
    contract = (((0,), (0,)), ((), ()))
    grad_down = lax.dot_general(hidden, grads_in, contract, preferred_element_type=jnp.float32).astype(jnp.bfloat16)
    grad_gate = lax.dot_general(gate_grad, rows_in, contract, preferred_element_type=jnp.float32).astype(jnp.bfloat16)
    grad_up = lax.dot_general(up_grad, rows_in, contract, preferred_element_type=jnp.float32).astype(jnp.bfloat16)
    input_sums = block_sum((gate_grad, up_grad), (gate_w, up_w))
    return (grad_gate, grad_up, grad_down, input_sums)

def to_experts(per_source, capacity):
    width = per_source.shape[2]
    arranged = per_source.reshape(N_EP, EXPERTS, capacity, width).transpose(1, 0, 2, 3)
    return arranged.reshape(EXPERTS, N_EP * capacity, width)

def to_sources(per_expert, capacity):
    width = per_expert.shape[2]
    arranged = per_expert.reshape(EXPERTS, N_EP, capacity, width).transpose(1, 0, 2, 3)
    return arranged.reshape(N_EP, EXPERTS * capacity, width)

def reference(tokens, expert_ids, route_share, w_gate, w_up, w_down, reward_head, upstream, pair_order):
    capacity = TOK_DEV * TOPK // EXPERTS
    token_blocks = tokens.reshape(N_EP, TOK_DEV, D).astype(jnp.float32)
    picker, mixing = jax.vmap(partial(route_tables, capacity=capacity))(expert_ids.reshape(N_EP, TOK_DEV, TOPK), route_share.reshape(N_EP, TOK_DEV))
    gathered = jnp.einsum('pts,ptd->psd', picker, token_blocks, precision=highest)
    slot_inputs = to_experts(gathered.astype(jnp.bfloat16), capacity)
    gate_all = w_gate.reshape(EXPERTS, FF, D)
    up_all = w_up.reshape(EXPERTS, FF, D)
    down_all = w_down.reshape(EXPERTS, FF, D)
    expert_out = lax.map(expert_forward, (slot_inputs, gate_all, up_all, down_all))
    mixed_sum = jnp.einsum('pts,psd->ptd', mixing, to_sources(expert_out, capacity), precision=highest)
    layer_out = (token_blocks + mixed_sum).astype(jnp.bfloat16).reshape(TOKENS, D)
    scores = jnp.dot(layer_out.astype(jnp.float32), reward_head, precision=highest)
    rewards = lax.optimization_barrier(jnp.sum(scores.reshape(SEQS, SEQ_LEN), axis=1)) / math.sqrt(SEQ_LEN)
    seq_iota = jnp.arange(SEQS, dtype=jnp.int32)
    chosen_hot = (pair_order[0::2][:, None] == seq_iota[None, :]).astype(jnp.float32)
    rejected_hot = (pair_order[1::2][:, None] == seq_iota[None, :]).astype(jnp.float32)
    margin = jnp.dot(chosen_hot, rewards, precision=highest) - jnp.dot(rejected_hot, rewards, precision=highest)
    pair_loss = jnp.mean(jax.nn.softplus(-margin))
    pair_weight = jax.nn.sigmoid(-margin)
    seq_coef = jnp.dot(pair_weight, rejected_hot - chosen_hot, precision=highest)
    token_coef = jnp.repeat(seq_coef, SEQ_LEN)
    grad_out = (upstream.astype(jnp.float32) + loss_scale * token_coef[:, None] * reward_head[None, :] / math.sqrt(SEQ_LEN)).astype(jnp.bfloat16)
    grad_blocks = grad_out.reshape(N_EP, TOK_DEV, D).astype(jnp.float32)
    slot_grads = to_experts(jnp.einsum('pts,ptd->psd', mixing, grad_blocks, precision=highest).astype(jnp.bfloat16), capacity)
    grad_gate, grad_up, grad_down, input_sums = lax.map(expert_backward, (slot_inputs, slot_grads, gate_all, up_all, down_all))
    returned = jnp.einsum('pts,psd->ptd', picker, to_sources(input_sums, capacity), precision=highest)
    grad_tokens = (grad_blocks + returned).astype(jnp.bfloat16).reshape(TOKENS, D)
    return (layer_out, rewards, pair_loss, grad_tokens, grad_gate.reshape(EXPERTS * FF, D), grad_up.reshape(EXPERTS * FF, D), grad_down.reshape(EXPERTS * FF, D))
```

```python
import functools
import math

import jax
import jax.numpy as jnp
from jax import lax
from jax.experimental import pallas as pl
from jax.experimental.pallas import tpu as pltpu
from jax.sharding import Mesh
from jax.sharding import PartitionSpec as P

EXPERTS = 8
SEQ_LEN = 64
EP = ("ep_x", "ep_z")
TP = ("tp_y", "tp_c")
EP_TP = EP + TP


loss_scale = 256.0
bf16, f32 = jnp.bfloat16, jnp.float32


def route_tables(expert_ids, route_share, capacity):
    experts_iota = jnp.arange(EXPERTS, dtype=jnp.int32)
    first_hot = (expert_ids[:, 0:1] == experts_iota[None, :]).astype(jnp.int32)
    second_hot = (expert_ids[:, 1:2] == experts_iota[None, :]).astype(jnp.int32)
    first_rank = jnp.sum((jnp.cumsum(first_hot, axis=0) - first_hot) * first_hot, axis=1)
    second_before = (
        jnp.cumsum(second_hot, axis=0) - second_hot + jnp.sum(first_hot, axis=0)[None, :]
    )
    second_rank = jnp.sum(second_before * second_hot, axis=1)
    route_ranks = jnp.stack([first_rank, second_rank], axis=1)
    route_kept = route_ranks < capacity
    slot_index = jnp.where(route_kept, expert_ids * capacity + route_ranks, -1)
    shares = jnp.stack([route_share, 1.0 - route_share], axis=1) * route_kept.astype(f32)
    slot_iota = jnp.arange(EXPERTS * capacity, dtype=jnp.int32)
    matches = (slot_index[:, :, None] == slot_iota[None, None, :]).astype(f32)
    picker = jnp.sum(matches, axis=1)
    mixing = jnp.sum(matches * shares[:, :, None], axis=1)
    return (picker, mixing)


def rot(value, shift):
    return lax.ppermute(value, "tp_y", [(i, (i + shift) % 4) for i in range(4)])


def swap(value):
    return lax.ppermute(value, "tp_c", [(0, 1), (1, 0)])


def exchange(blocks):
    arrived = lax.all_to_all(
        blocks.transpose(1, 0, 2), EP, split_axis=1, concat_axis=1, tiled=True
    )
    return arrived.transpose(1, 0, 2)


def gather_features(rows):
    half = rows.shape[0] // 2
    low, high = rows[:half], rows[half:]
    back_low, ahead_high = rot(low, 1), rot(high, -1)
    back_high, ahead_low = rot(high, 1), rot(low, -1)
    far_low, far_high = rot(back_low, 1), rot(ahead_high, -1)
    return (rows, ahead_low, ahead_high, far_low, far_high, back_low, back_high)


def add(*terms):
    return sum((t.astype(f32) for t in terms[1:]), terms[0].astype(f32)).astype(bf16)


def scatter_features(pieces):
    own, ahead_low, ahead_high, far_low, far_high, back_low, back_high = pieces
    half = far_low.shape[0]
    via_low, via_high = rot(far_low, 1), rot(far_high, -1)
    one_high, one_low = rot(ahead_high, 1), rot(back_low, -1)
    two_low = rot(add(ahead_low, via_low), 1)
    two_high = rot(add(back_high, via_high), -1)
    return jnp.concatenate(
        [add(own[:half], two_low, one_low), add(own[half:], one_high, two_high)], axis=0
    )


def load_piece(step, refs, rows):
    half = rows.shape[0] // 2
    own, ahead_low, ahead_high, far_low, far_high, back_low, back_high = refs
    pairs = (
        (own.at[pl.ds(0, half)], own.at[pl.ds(half, half)]),
        (ahead_low, ahead_high),
        (far_low, far_high),
        (back_low, back_high),
    )
    for k, (low, high) in enumerate(pairs):

        @pl.when(step == k)
        def _(low=low, high=high):
            rows[pl.ds(0, half)] = low[...]
            rows[pl.ds(half, half)] = high[...]


def store_piece(step, refs, rows):
    half = rows.shape[0] // 2
    own, ahead_low, ahead_high, far_low, far_high, back_low, back_high = refs
    pairs = (
        (own.at[pl.ds(0, half)], own.at[pl.ds(half, half)]),
        (ahead_low, ahead_high),
        (far_low, far_high),
        (back_low, back_high),
    )
    for k, (low, high) in enumerate(pairs):

        @pl.when(step == k)
        def _(low=low, high=high):
            low[...] = rows[pl.ds(0, half)]
            high[...] = rows[pl.ds(half, half)]


def cross(a, b):
    return lax.dot_general(a, b, (((1,), (1,)), ((), ())), preferred_element_type=f32)


def plain(a, b):
    return lax.dot_general(a, b, (((1,), (0,)), ((), ())), preferred_element_type=f32)


def fwd_kernel(y_ref, *refs):
    x_refs = refs[:7]
    wg0, wg1, wu0, wu1, wd0, wd1, rh_ref = refs[7:14]
    slope_ref, silu_ref, hidden_ref, score_ref = refs[14:18]
    out_refs = refs[18:25]
    gate_acc, up_acc, rows = refs[25:]
    half, width = gate_acc.shape[0] // 2, wg0.shape[0]
    left, right = pl.ds(0, width), pl.ds(width, width)
    step = pl.program_id(0)

    @pl.when(step == 0)
    def _():
        gate_acc[...] = jnp.zeros_like(gate_acc)
        up_acc[...] = jnp.zeros_like(up_acc)

    @pl.when(step < 4)
    def _():
        load_piece(step, x_refs, rows)
        gate_acc[:, left] += cross(rows[...], wg0[...])
        gate_acc[:, right] += cross(rows[...], wg1[...])
        up_acc[:, left] += cross(rows[...], wu0[...])
        up_acc[:, right] += cross(rows[...], wu1[...])

    @pl.when(step == 3)
    def _():
        for i in range(4):
            at = pl.ds(i * half // 2, half // 2)
            gate, up = gate_acc[at], up_acc[at]
            sig = jax.nn.sigmoid(gate)
            silu = gate * sig
            hidden = (silu * up).astype(bf16)
            silu_ref[at] = silu
            slope_ref[at] = up * (sig * (1.0 + gate * (1.0 - sig)))
            hidden_ref[at] = hidden
            score_ref[at] = jnp.sum(hidden.astype(f32) * rh_ref[...], axis=1, keepdims=True)

    @pl.when(step >= 4)
    def _():
        rows[...] = (
            plain(hidden_ref[:, left], wd0[...]) + plain(hidden_ref[:, right], wd1[...])
        ).astype(bf16)
        store_piece(step - 4, out_refs, rows)


def bwd_kernel(y_ref, *refs):
    u_refs = refs[:7]
    wg0, wg1, wu0, wu1, wd0, wd1, rh_ref, coef_ref, slope_ref, silu_ref = refs[7:17]
    gate_grad_ref, up_grad_ref = refs[17:19]
    out_refs = refs[19:26]
    acc, rows = refs[26:]
    half, width = acc.shape[0] // 2, wg0.shape[0]
    left, right = pl.ds(0, width), pl.ds(width, width)
    step = pl.program_id(0)

    @pl.when(step == 0)
    def _():
        acc[...] = jnp.zeros_like(acc)

    @pl.when(step < 4)
    def _():
        load_piece(step, u_refs, rows)
        acc[:, left] += cross(rows[...], wd0[...])
        acc[:, right] += cross(rows[...], wd1[...])

    @pl.when(step == 3)
    def _():
        for i in range(4):
            at = pl.ds(i * half // 2, half // 2)
            hidden_grad = acc[at] + coef_ref[at] * rh_ref[...]
            gate_grad_ref[at] = (hidden_grad * slope_ref[at]).astype(bf16)
            up_grad_ref[at] = (hidden_grad * silu_ref[at]).astype(bf16)

    @pl.when(step >= 4)
    def _():
        rows[...] = (
            plain(gate_grad_ref[:, left], wg0[...])
            + plain(gate_grad_ref[:, right], wg1[...])
            + plain(up_grad_ref[:, left], wu0[...])
            + plain(up_grad_ref[:, right], wu1[...])
        ).astype(bf16)
        store_piece(step - 4, out_refs, rows)


def grad_kernel(y_ref, *refs):
    x_refs, u_refs = refs[:7], refs[7:14]
    hidden_ref, gate_grad_ref, up_grad_ref, coef_ref, rh_ref = refs[14:19]
    own_refs, other_refs = refs[19:22], refs[22:25]
    left, rows = refs[25:]
    width = own_refs[0].shape[0]
    step = pl.program_id(0)

    @pl.when(step == 0)
    def _():
        for i, ref in enumerate((gate_grad_ref, up_grad_ref, hidden_ref)):
            left[i] = ref[...].T

    load_piece(step, x_refs, rows)
    for i in (0, 1):
        total = plain(left[i], rows[...])
        own_refs[i][...] = total[:width].astype(bf16)
        other_refs[i][...] = total[width:].astype(bf16)
    load_piece(step, u_refs, rows)
    rows[...] = (rows[...].astype(f32) + coef_ref[...] * rh_ref[...]).astype(bf16)
    total = plain(left[2], rows[...])
    own_refs[2][...] = total[:width].astype(bf16)
    other_refs[2][...] = total[width:].astype(bf16)


def whole(shape):
    return pl.BlockSpec(shape, lambda k, y: (0,) * len(shape))


def first_columns(width, block):
    return pl.BlockSpec((width, block), lambda k, y: (0, (y[0] + jnp.minimum(k, 3)) % 4))


def last_columns(width, block):
    return pl.BlockSpec((width, block), lambda k, y: (0, (y[0] + jnp.maximum(k - 4, 0)) % 4))


def all_columns(width, block):
    return pl.BlockSpec((width, block), lambda k, y: (0, (y[0] + k) % 4))


def piece_specs(rows, block):
    return [whole((rows, block))] + [whole((rows // 2, block))] * 6


def piece_shapes(rows, block):
    return [jax.ShapeDtypeStruct((rows, block), bf16)] + [
        jax.ShapeDtypeStruct((rows // 2, block), bf16)
    ] * 6


def call(kernel, steps, in_specs, out_specs, out_shape, scratch, flops, args):
    return pl.pallas_call(
        kernel,
        grid_spec=pltpu.PrefetchScalarGridSpec(
            num_scalar_prefetch=1,
            grid=(steps,),
            in_specs=in_specs,
            out_specs=out_specs,
            scratch_shapes=scratch,
        ),
        out_shape=out_shape,
        compiler_params=pltpu.CompilerParams(
            dimension_semantics=("arbitrary",), vmem_limit_bytes=56 * 1024 * 1024
        ),
        cost_estimate=pl.CostEstimate(flops=flops, bytes_accessed=20_000_000, transcendentals=0),
    )(*args)


def per_device(
    tokens, expert_ids, route_share, w_gate, w_up, w_down, reward_head, upstream, pair_order
):
    tok_count, local_width = tokens.shape
    capacity = tok_count * expert_ids.shape[1] // EXPERTS
    ep_size = lax.axis_size(EP)
    replicas = ep_size // EXPERTS
    half_cap = capacity // 2
    block = 2 * local_width
    rows = ep_size * half_cap
    hid = w_gate.shape[0]
    core = lax.axis_index("tp_c")
    place = lax.axis_index("tp_y").astype(jnp.int32).reshape(1)

    wg_other, wu_other, wd_other = swap(w_gate), swap(w_up), swap(w_down)

    picker, mixing = route_tables(expert_ids, route_share, capacity)
    slot_share = jnp.sum(mixing, axis=0)
    seq_local = tok_count // SEQ_LEN
    seq_share = jnp.sum(mixing.reshape(seq_local, SEQ_LEN, -1), axis=1)
    both = lax.dot_general(
        picker.astype(bf16),
        jnp.concatenate([tokens, upstream], axis=1),
        (((0,), (0,)), ((), ())),
        preferred_element_type=f32,
    )
    scale = jnp.concatenate(
        [jnp.ones_like(tokens[:1], f32), jnp.zeros_like(tokens[:1], f32)], axis=1
    )
    both = (both * (scale + (1.0 - scale) * slot_share[:, None])).astype(bf16)
    both = both.reshape(EXPERTS, 2, half_cap, 2 * local_width)
    mine = lax.dynamic_index_in_dim(both, core, 1, keepdims=False)
    theirs = swap(lax.dynamic_index_in_dim(both, 1 - core, 1, keepdims=False))
    low = jnp.where(core == 0, mine, theirs)
    high = jnp.where(core == 0, theirs, mine)
    token_block = jnp.concatenate([low[..., :local_width], high[..., :local_width]], axis=-1)
    grad_block = jnp.concatenate([low[..., local_width:], high[..., local_width:]], axis=-1)

    share_high = lax.reduce_precision(seq_share, 8, 7)
    share_low = seq_share - share_high
    meta = jnp.stack([share_high[0], share_low[0], share_high[1], share_low[1]], axis=1)
    meta = meta.reshape(EXPERTS, 2, half_cap, 4)
    meta = lax.dynamic_index_in_dim(meta, core, 1, keepdims=False).astype(bf16)
    meta = jnp.pad(meta, ((0, 0), (0, 0), (0, 124)))
    grad_block = jnp.concatenate([grad_block, meta], axis=-1)

    token_rows = exchange(jnp.repeat(token_block, replicas, axis=0)).reshape(rows, block)
    grad_rows = exchange(jnp.repeat(grad_block, replicas, axis=0))
    share_rows = grad_rows[:, :, block : block + 4].astype(f32)
    slot_shares = jnp.stack(
        [share_rows[..., 0] + share_rows[..., 1], share_rows[..., 2] + share_rows[..., 3]],
        axis=-1,
    )
    grad_rows = grad_rows[:, :, :block].reshape(rows, block)

    token_pieces = gather_features(token_rows)
    grad_pieces = gather_features(grad_rows)

    head = lax.all_gather(reward_head, TP, axis=0, tiled=True)
    head_own = jnp.sum(w_down.astype(f32) * head[None, :], axis=1)
    head_other = jnp.sum(wd_other.astype(f32) * head[None, :], axis=1)
    head_row = jnp.concatenate([head_own, head_other])[None, :]

    slots_hid = (rows, 2 * hid)
    weights = (w_gate, wg_other, w_up, wu_other, w_down, wd_other)
    outs = call(
        fwd_kernel,
        8,
        piece_specs(rows, block)
        + [first_columns(hid, block)] * 4
        + [last_columns(hid, block)] * 2
        + [whole((1, 2 * hid))],
        [whole(slots_hid)] * 3 + [whole((rows, 1))] + piece_specs(rows, block),
        [jax.ShapeDtypeStruct(slots_hid, f32)] * 2
        + [jax.ShapeDtypeStruct(slots_hid, bf16), jax.ShapeDtypeStruct((rows, 1), f32)]
        + piece_shapes(rows, block),
        [pltpu.VMEM(slots_hid, f32)] * 2 + [pltpu.VMEM((rows, block), bf16)],
        6 * rows * 2 * hid * 4 * block,
        (place, *token_pieces, *weights, head_row),
    )
    slope, silu, hidden, score = outs[:4]

    local_scores = jnp.sum(tokens.astype(f32) * reward_head[None, :], axis=1)
    local_rewards = jnp.sum(local_scores.reshape(seq_local, SEQ_LEN), axis=1)
    seq_total = pair_order.shape[0]
    offset = lax.axis_index(EP) * seq_local
    placed = lax.dynamic_update_slice(jnp.zeros((seq_total,), f32), local_rewards, (offset,))
    slot_scores = jnp.sum(slot_shares * score.reshape(ep_size, half_cap, 1), axis=1)
    placed = placed + slot_scores.reshape(seq_total)
    for axis in ("tp_c", "tp_y", "ep_x", "ep_z"):
        placed = lax.psum(placed, axis)
    rewards = placed / math.sqrt(SEQ_LEN)

    seq_iota = jnp.arange(seq_total, dtype=jnp.int32)
    chosen_hot = (pair_order[0::2][:, None] == seq_iota[None, :]).astype(f32)
    rejected_hot = (pair_order[1::2][:, None] == seq_iota[None, :]).astype(f32)
    margin = jnp.sum((chosen_hot - rejected_hot) * rewards[None, :], axis=1)
    pair_loss = jnp.mean(jax.nn.softplus(-margin))
    pair_weight = jax.nn.sigmoid(-margin)
    seq_coef = jnp.sum(pair_weight[:, None] * (rejected_hot - chosen_hot), axis=0)
    token_coef = jnp.repeat(lax.dynamic_slice_in_dim(seq_coef, offset, seq_local), SEQ_LEN)
    grad_out = (
        upstream.astype(f32)
        + loss_scale * token_coef[:, None] * reward_head[None, :] / math.sqrt(SEQ_LEN)
    ).astype(bf16)
    slot_coef = jnp.sum(slot_shares * seq_coef.reshape(ep_size, 1, seq_local), axis=-1)
    slot_coef = (slot_coef * (loss_scale / math.sqrt(SEQ_LEN))).reshape(rows, 1)

    outs_bwd = call(
        bwd_kernel,
        8,
        piece_specs(rows, block)
        + [last_columns(hid, block)] * 4
        + [first_columns(hid, block)] * 2
        + [whole((1, 2 * hid)), whole((rows, 1)), whole(slots_hid), whole(slots_hid)],
        [whole(slots_hid)] * 2 + piece_specs(rows, block),
        [jax.ShapeDtypeStruct(slots_hid, bf16)] * 2 + piece_shapes(rows, block),
        [pltpu.VMEM(slots_hid, f32), pltpu.VMEM((rows, block), bf16)],
        6 * rows * 2 * hid * 4 * block,
        (place, *grad_pieces, *weights, head_row, slot_coef, slope, silu),
    )
    gate_grad, up_grad = outs_bwd[:2]

    grads = call(
        grad_kernel,
        4,
        piece_specs(rows, block) * 2
        + [whole(slots_hid)] * 3
        + [whole((rows, 1)), all_columns(1, block)],
        [all_columns(hid, block)] * 6,
        [jax.ShapeDtypeStruct((hid, 4 * block), bf16)] * 6,
        [pltpu.VMEM((3, 2 * hid, rows), bf16), pltpu.VMEM((rows, block), bf16)],
        6 * rows * 2 * hid * 4 * block,
        (place, *token_pieces, *grad_pieces, hidden, gate_grad, up_grad, slot_coef, head[None, :]),
    )
    grad_gate, grad_up, grad_down = (add(own, swap(other)) for own, other in zip(grads[:3], grads[3:]))

    def come_back(pieces):
        summed = scatter_features(pieces).reshape(ep_size, half_cap, block)
        arrived = exchange(summed).astype(f32).reshape(EXPERTS, replicas, half_cap, block)
        sums = jnp.sum(arrived, axis=1).astype(bf16)
        halves = sums.reshape(EXPERTS, half_cap, 2, local_width)
        mine = lax.dynamic_index_in_dim(halves, core, 2, keepdims=False)
        theirs = swap(lax.dynamic_index_in_dim(halves, 1 - core, 2, keepdims=False))
        both = jnp.stack(
            [jnp.where(core == 0, mine, theirs), jnp.where(core == 0, theirs, mine)], axis=1
        )
        return both.reshape(EXPERTS * capacity, local_width)

    mixed_sum = plain(mixing, come_back(outs[4:]).astype(f32))
    layer_out = (tokens.astype(f32) + mixed_sum).astype(bf16)
    returned = plain(picker.astype(bf16), come_back(outs_bwd[2:]))
    grad_tokens = (grad_out.astype(f32) + returned).astype(bf16)
    return (layer_out, rewards, pair_loss, grad_tokens, grad_gate, grad_up, grad_down)


def solution(mesh):
    split = Mesh(mesh.devices.reshape(4, 8, 4, 2), EP_TP)
    in_specs = (
        P(EP, TP),
        P(EP, None),
        P(EP),
        P(EP_TP, None),
        P(EP_TP, None),
        P(EP_TP, None),
        P(TP),
        P(EP, TP),
        P(),
    )
    out_specs = (P(EP, TP), P(), P(), P(EP, TP), P(EP_TP, None), P(EP_TP, None), P(EP_TP, None))
    return jax.shard_map(
        per_device, mesh=split, in_specs=in_specs, out_specs=out_specs, check_vma=False
    )
```

```python
import math

import jax
import jax.numpy as jnp
from jax import lax
from jax.experimental import pallas as pl
from jax.experimental.pallas import tpu as pltpu
from jax.sharding import Mesh
from jax.sharding import PartitionSpec as P


EXPERTS = 8
SEQ_LEN = 64
EP = ("ep_x", "ep_z")
TP = ("tp_y", "tp_c")
EP_TP = EP + TP


loss_scale = 256.0
bf16, f32 = jnp.bfloat16, jnp.float32


def route_tables(expert_ids, route_share, capacity):
    experts_iota = jnp.arange(EXPERTS, dtype=jnp.int32)
    first_hot = (expert_ids[:, 0:1] == experts_iota[None, :]).astype(jnp.int32)
    second_hot = (expert_ids[:, 1:2] == experts_iota[None, :]).astype(jnp.int32)
    first_rank = jnp.sum((jnp.cumsum(first_hot, axis=0) - first_hot) * first_hot, axis=1)
    second_before = (
        jnp.cumsum(second_hot, axis=0) - second_hot + jnp.sum(first_hot, axis=0)[None, :]
    )
    second_rank = jnp.sum(second_before * second_hot, axis=1)
    route_ranks = jnp.stack([first_rank, second_rank], axis=1)
    route_kept = route_ranks < capacity
    half = capacity // 2
    slot_index = (route_ranks // half) * (EXPERTS * half) + expert_ids * half + route_ranks % half
    slot_index = jnp.where(route_kept, slot_index, -1)
    shares = jnp.stack([route_share, 1.0 - route_share], axis=1) * route_kept.astype(f32)
    slot_iota = jnp.arange(EXPERTS * capacity, dtype=jnp.int32)
    matches = (slot_index[:, :, None] == slot_iota[None, None, :]).astype(f32)
    picker = jnp.sum(matches, axis=1)
    mixing = jnp.sum(matches * shares[:, :, None], axis=1)
    return (picker, mixing)


def rot(value, shift):
    return lax.ppermute(value, "tp_y", [(i, (i + shift) % 4) for i in range(4)])


def swap(value):
    return lax.ppermute(value, "tp_c", [(0, 1), (1, 0)])


def exchange(blocks):
    arrived = lax.all_to_all(
        blocks.transpose(1, 0, 2), EP, split_axis=1, concat_axis=1, tiled=True
    )
    return arrived.transpose(1, 0, 2)


def gather_features(rows):
    half = rows.shape[0] // 2
    back, ahead = rot(rows, 1), rot(rows, -1)
    far_low, far_high = rot(back[:half], 1), rot(ahead[half:], -1)
    return (rows, ahead, far_low, far_high, back)


def add(*terms):
    return sum((t.astype(f32) for t in terms[1:]), terms[0].astype(f32)).astype(bf16)


def scatter_start(pieces):
    own, ahead, far_low, far_high, back = pieces
    half = far_low.shape[0]
    via_low, via_high = rot(far_low, 1), rot(far_high, -1)
    onward = jnp.concatenate([add(ahead[:half], via_low), ahead[half:]], axis=0)
    backward = jnp.concatenate([back[:half], add(back[half:], via_high)], axis=0)
    return own, rot(onward, 1), rot(backward, -1)


def piece_halves(refs):
    own, ahead, far_low, far_high, back = refs
    half = far_low.shape[0]
    low, high = pl.ds(0, half), pl.ds(half, half)
    return (
        (own.at[low], own.at[high]),
        (ahead.at[low], ahead.at[high]),
        (far_low, far_high),
        (back.at[low], back.at[high]),
    )


def load_piece(step, refs, rows):
    half = rows.shape[0] // 2
    for k, (low, high) in enumerate(piece_halves(refs)):

        @pl.when(step == k)
        def _(low=low, high=high):
            rows[pl.ds(0, half)] = low[...]
            rows[pl.ds(half, half)] = high[...]


def store_piece(step, refs, rows):
    half = rows.shape[0] // 2
    for k, (low, high) in enumerate(piece_halves(refs)):

        @pl.when(step == k)
        def _(low=low, high=high):
            low[...] = rows[pl.ds(0, half)]
            high[...] = rows[pl.ds(half, half)]


def cross(a, b):
    return lax.dot_general(a, b, (((1,), (1,)), ((), ())), preferred_element_type=f32)


def plain(a, b):
    return lax.dot_general(a, b, (((1,), (0,)), ((), ())), preferred_element_type=f32)


def fwd_kernel(y_ref, *refs):
    x_refs = refs[:5]
    wg0, wg1, wu0, wu1, rh_ref, meta_ref = refs[5:11]
    slope_ref, silu_ref, hidden_ref, score_ref = refs[11:15]
    gate_acc, up_acc, rows = refs[15:]
    width = wg0.shape[0]
    left, right = pl.ds(0, width), pl.ds(width, width)
    step = pl.program_id(0)

    @pl.when(step == 0)
    def _():
        gate_acc[...] = jnp.zeros_like(gate_acc)
        up_acc[...] = jnp.zeros_like(up_acc)

    load_piece(step, x_refs, rows)
    gate_acc[:, left] += cross(rows[...], wg0[...])
    gate_acc[:, right] += cross(rows[...], wg1[...])
    up_acc[:, left] += cross(rows[...], wu0[...])
    up_acc[:, right] += cross(rows[...], wu1[...])

    @pl.when(step == 3)
    def _():
        chunk = gate_acc.shape[0] // 8

        @pl.loop(0, 8)
        def _(i):
            at = pl.ds(pl.multiple_of(i * chunk, chunk), chunk)
            gate, up = gate_acc[at], up_acc[at]
            sig = jax.nn.sigmoid(gate)
            silu = gate * sig
            hidden = (silu * up).astype(bf16)
            silu_ref[at] = silu
            slope_ref[at] = up * (sig * (1.0 + gate * (1.0 - sig)))
            hidden_ref[at] = hidden
            score = jnp.sum(hidden.astype(f32) * rh_ref[...], axis=1, keepdims=True)
            gate_acc[at, pl.ds(0, 128)] = score * meta_ref[at].astype(f32)

        scores = gate_acc[:, pl.ds(0, 128)].reshape(score_ref.shape[0], -1, 128)
        scores = jnp.sum(scores, axis=1)
        lane = lax.broadcasted_iota(jnp.int32, scores.shape, 1)
        first = jnp.sum(jnp.where(lane < 2, scores, 0.0), axis=1, keepdims=True)
        second = jnp.sum(jnp.where(lane < 2, 0.0, scores), axis=1, keepdims=True)
        score_ref[...] = jnp.where(lane == 0, first, second)


def down_kernel(y_ref, hidden_ref, wd0, wd1, *refs):
    out_refs, rows = refs[:5], refs[5]
    width = wd0.shape[0]
    left, right = pl.ds(0, width), pl.ds(width, width)
    rows[...] = (
        plain(hidden_ref[:, left], wd0[...]) + plain(hidden_ref[:, right], wd1[...])
    ).astype(bf16)
    store_piece(pl.program_id(0), out_refs, rows)


def back_kernel(y_ref, *refs):
    u_refs, (wd0, wd1, out_ref, rows) = refs[:5], refs[5:]
    width = wd0.shape[0]
    left, right = pl.ds(0, width), pl.ds(width, width)
    step = pl.program_id(0)

    @pl.when(step == 0)
    def _():
        out_ref[...] = jnp.zeros_like(out_ref)

    load_piece(step, u_refs, rows)
    out_ref[:, left] += cross(rows[...], wd0[...])
    out_ref[:, right] += cross(rows[...], wd1[...])


def bwd_kernel(y_ref, *refs):
    wg0, wg1, wu0, wu1, rh_ref, meta_ref, seq_ref, partial_ref, slope_ref, silu_ref = refs[:10]
    gate_grad_ref, up_grad_ref, coef_ref = refs[10:13]
    out_refs, rows = refs[13:18], refs[18]
    width = wg0.shape[0]
    left, right = pl.ds(0, width), pl.ds(width, width)
    step = pl.program_id(0)

    @pl.when(step == 0)
    def _():
        count = partial_ref.shape[0]
        blocks = seq_ref.shape[0]
        lane = lax.broadcasted_iota(jnp.int32, (blocks, 128), 1)
        first = jnp.broadcast_to(seq_ref[:, pl.ds(0, 1)], lane.shape)
        second = jnp.broadcast_to(seq_ref[:, pl.ds(1, 1)], lane.shape)
        by_lane = jnp.where(lane < 2, first, jnp.where(lane < 4, second, 0.0))
        shares = meta_ref[...].astype(f32).reshape(blocks, count // blocks, 128)
        terms = (shares * by_lane[:, None, :]).reshape(count, 128)
        coef_ref[...] = jnp.sum(terms, axis=1, keepdims=True)
        chunk = count // 8

        @pl.loop(0, 8)
        def _(i):
            at = pl.ds(pl.multiple_of(i * chunk, chunk), chunk)
            hidden_grad = partial_ref[at] + coef_ref[at] * rh_ref[...]
            gate_grad_ref[at] = (hidden_grad * slope_ref[at]).astype(bf16)
            up_grad_ref[at] = (hidden_grad * silu_ref[at]).astype(bf16)

    rows[...] = (
        plain(gate_grad_ref[:, left], wg0[...])
        + plain(gate_grad_ref[:, right], wg1[...])
        + plain(up_grad_ref[:, left], wu0[...])
        + plain(up_grad_ref[:, right], wu1[...])
    ).astype(bf16)
    store_piece(step, out_refs, rows)


def grad_kernel(y_ref, *refs):
    x_refs, u_refs = refs[:5], refs[5:10]
    hidden_ref, gate_grad_ref, up_grad_ref, coef_ref, rh_ref = refs[10:15]
    own_refs, other_ref = refs[15:18], refs[18]
    left, rows = refs[19:]
    width = own_refs[0].shape[0]
    step = pl.program_id(0)

    @pl.when(step == 0)
    def _():
        for i, ref in enumerate((gate_grad_ref, up_grad_ref, hidden_ref)):
            left[i] = ref[...].T

    load_piece(step, x_refs, rows)
    for i in (0, 1, 2):
        if i == 2:
            load_piece(step, u_refs, rows)
            rows[...] = (rows[...].astype(f32) + coef_ref[...] * rh_ref[...]).astype(bf16)
        total = plain(left[i], rows[...])
        own_refs[i][...] = total[:width].astype(bf16)
        other_ref[pl.ds(i * width, width)] = total[width:].astype(bf16)


def whole(shape):
    return pl.BlockSpec(shape, lambda k, y: (0,) * len(shape))


def columns(width, block):
    return pl.BlockSpec((width, block), lambda k, y: (0, (y[0] + k) % 4))


def piece_specs(rows, block):
    full, part = whole((rows, block)), whole((rows // 2, block))
    return [full, full, part, part, full]


def piece_shapes(rows, block):
    full = jax.ShapeDtypeStruct((rows, block), bf16)
    part = jax.ShapeDtypeStruct((rows // 2, block), bf16)
    return [full, full, part, part, full]


def call(kernel, in_specs, out_specs, out_shape, scratch, flops, args):
    return pl.pallas_call(
        kernel,
        grid_spec=pltpu.PrefetchScalarGridSpec(
            num_scalar_prefetch=1,
            grid=(4,),
            in_specs=in_specs,
            out_specs=out_specs,
            scratch_shapes=scratch,
        ),
        out_shape=out_shape,
        compiler_params=pltpu.CompilerParams(
            dimension_semantics=("arbitrary",), vmem_limit_bytes=36 * 1024 * 1024
        ),
        cost_estimate=pl.CostEstimate(flops=flops, bytes_accessed=20_000_000, transcendentals=0),
    )(*args)


def layer(
    tokens, expert_ids, route_share, w_gate, w_up, w_down, reward_head, upstream, pair_order
):
    tok_count, local_width = tokens.shape
    capacity = tok_count * expert_ids.shape[1] // EXPERTS
    ep_size = lax.axis_size(EP)
    replicas = ep_size // EXPERTS
    half_cap = capacity // 2
    block = 2 * local_width
    rows = ep_size * half_cap
    hid = w_gate.shape[0]
    core = lax.axis_index("tp_c")
    place = lax.axis_index("tp_y").astype(jnp.int32).reshape(1)

    wg_other, wu_other, wd_other = swap(w_gate), swap(w_up), swap(w_down)

    picker, mixing = route_tables(expert_ids, route_share, capacity)
    seq_local = tok_count // SEQ_LEN
    over_tokens = (((0,), (0,)), ((), ()))
    both = lax.dot_general(
        picker.astype(bf16),
        jnp.concatenate([tokens, upstream], axis=1),
        over_tokens,
        preferred_element_type=f32,
    )
    slot_share = jnp.sum(mixing, axis=0)
    column = lax.broadcasted_iota(jnp.int32, (1, 2 * local_width), 1)
    both = both * jnp.where(column < local_width, 1.0, slot_share[:, None])
    both = both.astype(bf16).reshape(2, EXPERTS * half_cap, 2 * local_width)
    mine = lax.dynamic_index_in_dim(both, core, 0, keepdims=False)
    theirs = swap(lax.dynamic_index_in_dim(both, 1 - core, 0, keepdims=False))
    low = jnp.where(core == 0, mine, theirs)
    high = jnp.where(core == 0, theirs, mine)
    token_block = jnp.concatenate([low[:, :local_width], high[:, :local_width]], axis=1)
    grad_block = jnp.concatenate([low[:, local_width:], high[:, local_width:]], axis=1)

    token_seq = lax.broadcasted_iota(jnp.int32, (tok_count, 128), 0) // SEQ_LEN
    lane = lax.broadcasted_iota(jnp.int32, (tok_count, 128), 1)
    my_mixing = jnp.where(
        core == 0, mixing[:, : EXPERTS * half_cap], mixing[:, EXPERTS * half_cap :]
    )
    meta = lax.dot_general(
        my_mixing,
        (token_seq == lane // 2).astype(f32),
        over_tokens,
        precision=lax.Precision.HIGHEST,
        preferred_element_type=f32,
    )
    meta_high = lax.reduce_precision(meta, 8, 7)
    meta = jnp.where(lane[:1] % 2 == 0, meta_high, meta - meta_high).astype(bf16)
    grad_block = jnp.concatenate([grad_block, meta], axis=1)

    def to_experts(block_rows):
        width = block_rows.shape[1]
        block_rows = block_rows.reshape(EXPERTS, half_cap, width)
        return exchange(jnp.repeat(block_rows, replicas, axis=0)).reshape(rows, width)

    token_rows = to_experts(token_block)
    grad_full = to_experts(grad_block)

    head = lax.all_gather(reward_head, TP, axis=0, tiled=True)
    head_own = jnp.sum(w_down.astype(f32) * head[None, :], axis=1)
    head_other = jnp.sum(wd_other.astype(f32) * head[None, :], axis=1)
    head_row = jnp.concatenate([head_own, head_other])[None, :]
    local_scores = jnp.sum(tokens.astype(f32) * reward_head[None, :], axis=1)
    local_rewards = jnp.sum(local_scores.reshape(seq_local, SEQ_LEN), axis=1)
    seq_total = pair_order.shape[0]
    offset = lax.axis_index(EP) * seq_local
    placed = lax.dynamic_update_slice(jnp.zeros((seq_total,), f32), local_rewards, (offset,))
    token_rows, head_row, placed = lax.optimization_barrier((token_rows, head_row, placed))

    token_pieces = gather_features(token_rows)
    grad_pieces = gather_features(grad_full[:, :block])

    slots_hid = (rows, 2 * hid)
    meta_spec = pl.BlockSpec((rows, 128), lambda k, y: (0, block // 128))
    work = rows * 2 * hid * 4 * block
    slope, silu, hidden, score = call(
        fwd_kernel,
        piece_specs(rows, block)
        + [columns(hid, block)] * 4
        + [whole((1, 2 * hid)), meta_spec],
        [whole(slots_hid)] * 3 + [whole((ep_size, 128))],
        [jax.ShapeDtypeStruct(slots_hid, f32)] * 2
        + [jax.ShapeDtypeStruct(slots_hid, bf16), jax.ShapeDtypeStruct((ep_size, 128), f32)],
        [pltpu.VMEM(slots_hid, f32)] * 2 + [pltpu.VMEM((rows, block), bf16)],
        4 * work,
        (place, *token_pieces, w_gate, wg_other, w_up, wu_other, head_row, grad_full),
    )
    placed = (placed + score[:, :seq_local].reshape(seq_total)).reshape(2, 1, seq_total // 2)
    everyone = lax.axis_size(EP_TP)
    spread = jnp.broadcast_to(placed, (2, everyone, seq_total // 2))
    spread = lax.all_to_all(spread, EP_TP, split_axis=1, concat_axis=1, tiled=True)
    rewards = jnp.sum(spread, axis=1).reshape(seq_total) / math.sqrt(SEQ_LEN)

    down_pieces = call(
        down_kernel,
        [whole(slots_hid)] + [columns(hid, block)] * 2,
        piece_specs(rows, block),
        piece_shapes(rows, block),
        [pltpu.VMEM((rows, block), bf16)],
        2 * work,
        (place, hidden, w_down, wd_other),
    )
    partial = call(
        back_kernel,
        piece_specs(rows, block) + [columns(hid, block)] * 2,
        [whole(slots_hid)],
        [jax.ShapeDtypeStruct(slots_hid, f32)],
        [pltpu.VMEM((rows, block), bf16)],
        2 * work,
        (place, *grad_pieces, w_down, wd_other),
    )[0]
    down_sums = scatter_start(down_pieces)

    seq_iota = jnp.arange(seq_total, dtype=jnp.int32)
    chosen_hot = (pair_order[0::2][:, None] == seq_iota[None, :]).astype(f32)
    rejected_hot = (pair_order[1::2][:, None] == seq_iota[None, :]).astype(f32)
    margin = jnp.sum((chosen_hot - rejected_hot) * rewards[None, :], axis=1)
    pair_loss = jnp.mean(jax.nn.softplus(-margin))
    pair_weight = jax.nn.sigmoid(-margin)
    seq_coef = jnp.sum(pair_weight[:, None] * (rejected_hot - chosen_hot), axis=0)
    token_coef = jnp.repeat(lax.dynamic_slice_in_dim(seq_coef, offset, seq_local), SEQ_LEN)
    grad_out = (
        upstream.astype(f32)
        + loss_scale * token_coef[:, None] * reward_head[None, :] / math.sqrt(SEQ_LEN)
    ).astype(bf16)
    scaled = (seq_coef * (loss_scale / math.sqrt(SEQ_LEN))).reshape(ep_size, seq_local)

    gate_grad, up_grad, slot_coef, *input_pieces = call(
        bwd_kernel,
        [columns(hid, block)] * 4
        + [whole((1, 2 * hid)), meta_spec, whole((ep_size, seq_local))]
        + [whole(slots_hid)] * 3,
        [whole(slots_hid)] * 2 + [whole((rows, 1))] + piece_specs(rows, block),
        [jax.ShapeDtypeStruct(slots_hid, bf16)] * 2
        + [jax.ShapeDtypeStruct((rows, 1), f32)]
        + piece_shapes(rows, block),
        [pltpu.VMEM((rows, block), bf16)],
        4 * work,
        (place, w_gate, wg_other, w_up, wu_other, head_row, grad_full, scaled)
        + (partial, slope, silu),
    )
    input_sums = scatter_start(input_pieces)

    *own_grads, other_grads = call(
        grad_kernel,
        piece_specs(rows, block) * 2
        + [whole(slots_hid)] * 3
        + [whole((rows, 1)), columns(1, block)],
        [columns(hid, block)] * 3 + [columns(3 * hid, block)],
        [jax.ShapeDtypeStruct((hid, 4 * block), bf16)] * 3
        + [jax.ShapeDtypeStruct((3 * hid, 4 * block), bf16)],
        [pltpu.VMEM((3, 2 * hid, rows), bf16), pltpu.VMEM((rows, block), bf16)],
        6 * work,
        (place, *token_pieces, *grad_pieces, hidden, gate_grad, up_grad, slot_coef, head[None, :]),
    )
    other_grads = swap(other_grads)
    grad_gate, grad_up, grad_down = (
        add(own, other_grads[i * hid : (i + 1) * hid]) for i, own in enumerate(own_grads)
    )

    def come_back(pieces):
        arrived = exchange(add(*pieces).reshape(ep_size, half_cap, block)).astype(f32)
        sums = jnp.sum(arrived.reshape(EXPERTS, replicas, half_cap, block), axis=1)
        sums = sums.astype(bf16).reshape(EXPERTS * half_cap, block)
        left, right = sums[:, :local_width], sums[:, local_width:]
        mine = jnp.where(core == 0, left, right)
        theirs = swap(jnp.where(core == 0, right, left))
        return jnp.concatenate(
            [jnp.where(core == 0, mine, theirs), jnp.where(core == 0, theirs, mine)], axis=0
        )

    mixed_sum = plain(mixing, come_back(down_sums).astype(f32))
    layer_out = (tokens.astype(f32) + mixed_sum).astype(bf16)
    returned = plain(picker.astype(bf16), come_back(input_sums))
    grad_tokens = (grad_out.astype(f32) + returned).astype(bf16)
    return (layer_out, rewards, pair_loss, grad_tokens, grad_gate, grad_up, grad_down)


def solution(mesh):
    split = Mesh(mesh.devices.reshape(4, 8, 4, 2), EP_TP)
    in_specs = (
        P(EP, TP),
        P(EP, None),
        P(EP),
        P(EP_TP, None),
        P(EP_TP, None),
        P(EP_TP, None),
        P(TP),
        P(EP, TP),
        P(),
    )
    out_specs = (P(EP, TP), P(), P(), P(EP, TP), P(EP_TP, None), P(EP_TP, None), P(EP_TP, None))
    return jax.shard_map(layer, mesh=split, in_specs=in_specs, out_specs=out_specs, check_vma=False)
```

```python
import math

import jax
import jax.numpy as jnp
from jax import lax
from jax.experimental import pallas as pl
from jax.experimental.pallas import tpu as pltpu
from jax.sharding import Mesh
from jax.sharding import PartitionSpec as P


EXPERTS = 8
SEQ_LEN = 64
EP = ("ep_x", "ep_z")
TP = ("tp_y", "tp_c")
EP_TP = EP + TP


loss_scale = 256.0
VMEM_MIB = 60
bf16, f32 = jnp.bfloat16, jnp.float32


def route_tables(expert_ids, route_share, capacity):
    experts_iota = jnp.arange(EXPERTS, dtype=jnp.int32)
    first_hot = (expert_ids[:, 0:1] == experts_iota[None, :]).astype(jnp.int32)
    second_hot = (expert_ids[:, 1:2] == experts_iota[None, :]).astype(jnp.int32)
    first_rank = jnp.sum((jnp.cumsum(first_hot, axis=0) - first_hot) * first_hot, axis=1)
    second_before = (
        jnp.cumsum(second_hot, axis=0) - second_hot + jnp.sum(first_hot, axis=0)[None, :]
    )
    second_rank = jnp.sum(second_before * second_hot, axis=1)
    route_ranks = jnp.stack([first_rank, second_rank], axis=1)
    route_kept = route_ranks < capacity
    half = capacity // 2
    slot_index = (route_ranks // half) * (EXPERTS * half) + expert_ids * half + route_ranks % half
    slot_index = jnp.where(route_kept, slot_index, -1)
    shares = jnp.stack([route_share, 1.0 - route_share], axis=1) * route_kept.astype(f32)
    slot_iota = jnp.arange(EXPERTS * capacity, dtype=jnp.int32)
    matches = (slot_index[:, :, None] == slot_iota[None, None, :]).astype(f32)
    picker = jnp.sum(matches, axis=1)
    mixing = jnp.sum(matches * shares[:, :, None], axis=1)
    return (picker, mixing)


def rot(value, shift):
    return lax.ppermute(value, "tp_y", [(i, (i + shift) % 4) for i in range(4)])


def swap(value):
    return lax.ppermute(value, "tp_c", [(0, 1), (1, 0)])


def exchange(blocks):
    arrived = lax.all_to_all(
        blocks.transpose(1, 0, 2), EP, split_axis=1, concat_axis=1, tiled=True
    )
    return arrived.transpose(1, 0, 2)


def gather_features(rows):
    half = rows.shape[0] // 2
    back, ahead = rot(rows, 1), rot(rows, -1)
    far_low, far_high = rot(back[:half], 1), rot(ahead[half:], -1)
    return (rows, ahead, far_low, far_high, back)


def add(*terms):
    return sum((t.astype(f32) for t in terms[1:]), terms[0].astype(f32)).astype(bf16)


def scatter_start(pieces):
    own, ahead, far_low, far_high, back = pieces
    half = far_low.shape[0]
    via_low, via_high = rot(far_low, 1), rot(far_high, -1)
    onward = jnp.concatenate([add(ahead[:half], via_low), ahead[half:]], axis=0)
    backward = jnp.concatenate([back[:half], add(back[half:], via_high)], axis=0)
    return own, rot(onward, 1), rot(backward, -1)


def piece_halves(refs):
    own, ahead, far_low, far_high, back = refs
    half = far_low.shape[0]
    low, high = pl.ds(0, half), pl.ds(half, half)
    return (
        (own.at[low], own.at[high]),
        (ahead.at[low], ahead.at[high]),
        (far_low, far_high),
        (back.at[low], back.at[high]),
    )


def load_piece(step, refs, rows):
    half = rows.shape[0] // 2
    for k, (low, high) in enumerate(piece_halves(refs)):

        @pl.when(step == k)
        def _(low=low, high=high):
            rows[pl.ds(0, half)] = low[...]
            rows[pl.ds(half, half)] = high[...]


def store_piece(step, refs, rows):
    half = rows.shape[0] // 2
    for k, (low, high) in enumerate(piece_halves(refs)):

        @pl.when(step == k)
        def _(low=low, high=high):
            low[...] = rows[pl.ds(0, half)]
            high[...] = rows[pl.ds(half, half)]


def cross(a, b):
    return lax.dot_general(a, b, (((1,), (1,)), ((), ())), preferred_element_type=f32)


def plain(a, b):
    return lax.dot_general(a, b, (((1,), (0,)), ((), ())), preferred_element_type=f32)


def fwd_kernel(y_ref, *refs):
    x_refs = refs[:5]
    wg0, wg1, wu0, wu1, rh_ref, meta_ref = refs[5:11]
    slope_ref, silu_ref, hidden_ref, score_ref = refs[11:15]
    gate_acc, up_acc, rows = refs[15:]
    width = wg0.shape[0]
    left, right = pl.ds(0, width), pl.ds(width, width)
    step = pl.program_id(0)

    @pl.when(step == 0)
    def _():
        gate_acc[...] = jnp.zeros_like(gate_acc)
        up_acc[...] = jnp.zeros_like(up_acc)

    load_piece(step, x_refs, rows)
    gate_acc[:, left] += cross(rows[...], wg0[...])
    gate_acc[:, right] += cross(rows[...], wg1[...])
    up_acc[:, left] += cross(rows[...], wu0[...])
    up_acc[:, right] += cross(rows[...], wu1[...])

    @pl.when(step == 3)
    def _():
        chunk = gate_acc.shape[0] // 8

        @pl.loop(0, 8)
        def _(i):
            at = pl.ds(pl.multiple_of(i * chunk, chunk), chunk)
            gate, up = gate_acc[at], up_acc[at]
            sig = jax.nn.sigmoid(gate)
            silu = gate * sig
            hidden = (silu * up).astype(bf16)
            silu_ref[at] = silu
            slope_ref[at] = up * (sig * (1.0 + gate * (1.0 - sig)))
            hidden_ref[at] = hidden
            score = jnp.sum(hidden.astype(f32) * rh_ref[...], axis=1, keepdims=True)
            gate_acc[at, pl.ds(0, 128)] = score * meta_ref[at].astype(f32)

        scores = gate_acc[:, pl.ds(0, 128)].reshape(score_ref.shape[0], -1, 128)
        scores = jnp.sum(scores, axis=1)
        lane = lax.broadcasted_iota(jnp.int32, scores.shape, 1)
        first = jnp.sum(jnp.where(lane < 2, scores, 0.0), axis=1, keepdims=True)
        second = jnp.sum(jnp.where(lane < 2, 0.0, scores), axis=1, keepdims=True)
        score_ref[...] = jnp.where(lane == 0, first, second)


def down_kernel(y_ref, hidden_ref, wd0, wd1, *refs):
    out_refs, rows = refs[:5], refs[5]
    width = wd0.shape[0]
    left, right = pl.ds(0, width), pl.ds(width, width)
    rows[...] = (
        plain(hidden_ref[:, left], wd0[...]) + plain(hidden_ref[:, right], wd1[...])
    ).astype(bf16)
    store_piece(pl.program_id(0), out_refs, rows)


def back_kernel(y_ref, *refs):
    u_refs, (wd0, wd1, out_ref, rows) = refs[:5], refs[5:]
    width = wd0.shape[0]
    left, right = pl.ds(0, width), pl.ds(width, width)
    step = pl.program_id(0)

    @pl.when(step == 0)
    def _():
        out_ref[...] = jnp.zeros_like(out_ref)

    load_piece(step, u_refs, rows)
    out_ref[:, left] += cross(rows[...], wd0[...])
    out_ref[:, right] += cross(rows[...], wd1[...])


def bwd_kernel(y_ref, *refs):
    wg0, wg1, wu0, wu1, rh_ref, meta_ref, seq_ref, partial_ref, slope_ref, silu_ref = refs[:10]
    gate_grad_ref, up_grad_ref, coef_ref = refs[10:13]
    out_refs, rows = refs[13:18], refs[18]
    width = wg0.shape[0]
    left, right = pl.ds(0, width), pl.ds(width, width)
    step = pl.program_id(0)

    @pl.when(step == 0)
    def _():
        count = partial_ref.shape[0]
        blocks = seq_ref.shape[0]
        lane = lax.broadcasted_iota(jnp.int32, (blocks, 128), 1)
        first = jnp.broadcast_to(seq_ref[:, pl.ds(0, 1)], lane.shape)
        second = jnp.broadcast_to(seq_ref[:, pl.ds(1, 1)], lane.shape)
        by_lane = jnp.where(lane < 2, first, jnp.where(lane < 4, second, 0.0))
        shares = meta_ref[...].astype(f32).reshape(blocks, count // blocks, 128)
        terms = (shares * by_lane[:, None, :]).reshape(count, 128)
        coef_ref[...] = jnp.sum(terms, axis=1, keepdims=True)
        chunk = count // 8

        @pl.loop(0, 8)
        def _(i):
            at = pl.ds(pl.multiple_of(i * chunk, chunk), chunk)
            hidden_grad = partial_ref[at] + coef_ref[at] * rh_ref[...]
            gate_grad_ref[at] = (hidden_grad * slope_ref[at]).astype(bf16)
            up_grad_ref[at] = (hidden_grad * silu_ref[at]).astype(bf16)

    rows[...] = (
        plain(gate_grad_ref[:, left], wg0[...])
        + plain(gate_grad_ref[:, right], wg1[...])
        + plain(up_grad_ref[:, left], wu0[...])
        + plain(up_grad_ref[:, right], wu1[...])
    ).astype(bf16)
    store_piece(step, out_refs, rows)


def grad_kernel(y_ref, *refs):
    x_refs, u_refs = refs[:5], refs[5:10]
    hidden_ref, gate_grad_ref, up_grad_ref, coef_ref, rh_ref = refs[10:15]
    own_refs, other_ref = refs[15:18], refs[18]
    left, rows = refs[19:]
    width = own_refs[0].shape[0]
    step = pl.program_id(0)

    @pl.when(step == 0)
    def _():
        for i, ref in enumerate((gate_grad_ref, up_grad_ref, hidden_ref)):
            left[i] = ref[...].T

    load_piece(step, x_refs, rows)
    for i in (0, 1, 2):
        if i == 2:
            load_piece(step, u_refs, rows)
            rows[...] = (rows[...].astype(f32) + coef_ref[...] * rh_ref[...]).astype(bf16)
        total = plain(left[i], rows[...])
        own_refs[i][...] = total[:width].astype(bf16)
        other_ref[pl.ds(i * width, width)] = total[width:].astype(bf16)


def whole(shape):
    return pl.BlockSpec(shape, lambda k, y: (0,) * len(shape))


def columns(width, block):
    return pl.BlockSpec((width, block), lambda k, y: (0, (y[0] + k) % 4))


def piece_specs(rows, block):
    full, part = whole((rows, block)), whole((rows // 2, block))
    return [full, full, part, part, full]


def piece_shapes(rows, block):
    full = jax.ShapeDtypeStruct((rows, block), bf16)
    part = jax.ShapeDtypeStruct((rows // 2, block), bf16)
    return [full, full, part, part, full]


def call(kernel, in_specs, out_specs, out_shape, scratch, flops, args):
    return pl.pallas_call(
        kernel,
        grid_spec=pltpu.PrefetchScalarGridSpec(
            num_scalar_prefetch=1,
            grid=(4,),
            in_specs=in_specs,
            out_specs=out_specs,
            scratch_shapes=scratch,
        ),
        out_shape=out_shape,
        compiler_params=pltpu.CompilerParams(
            dimension_semantics=("arbitrary",), vmem_limit_bytes=VMEM_MIB * 1024 * 1024
        ),
        cost_estimate=pl.CostEstimate(flops=flops, bytes_accessed=20_000_000, transcendentals=0),
    )(*args)


def layer(
    tokens, expert_ids, route_share, w_gate, w_up, w_down, reward_head, upstream, pair_order
):
    tok_count, local_width = tokens.shape
    capacity = tok_count * expert_ids.shape[1] // EXPERTS
    ep_size = lax.axis_size(EP)
    replicas = ep_size // EXPERTS
    half_cap = capacity // 2
    block = 2 * local_width
    rows = ep_size * half_cap
    hid = w_gate.shape[0]
    core = lax.axis_index("tp_c")
    place = lax.axis_index("tp_y").astype(jnp.int32).reshape(1)

    wg_other, wu_other, wd_other = swap(w_gate), swap(w_up), swap(w_down)

    picker, mixing = route_tables(expert_ids, route_share, capacity)
    seq_local = tok_count // SEQ_LEN
    over_tokens = (((0,), (0,)), ((), ()))
    both = lax.dot_general(
        picker.astype(bf16),
        jnp.concatenate([tokens, upstream], axis=1),
        over_tokens,
        preferred_element_type=f32,
    )
    slot_share = jnp.sum(mixing, axis=0)
    column = lax.broadcasted_iota(jnp.int32, (1, 2 * local_width), 1)
    both = both * jnp.where(column < local_width, 1.0, slot_share[:, None])
    both = both.astype(bf16).reshape(2, EXPERTS * half_cap, 2 * local_width)
    mine = lax.dynamic_index_in_dim(both, core, 0, keepdims=False)
    theirs = swap(lax.dynamic_index_in_dim(both, 1 - core, 0, keepdims=False))
    low = jnp.where(core == 0, mine, theirs)
    high = jnp.where(core == 0, theirs, mine)
    token_block = jnp.concatenate([low[:, :local_width], high[:, :local_width]], axis=1)
    grad_block = jnp.concatenate([low[:, local_width:], high[:, local_width:]], axis=1)

    token_seq = lax.broadcasted_iota(jnp.int32, (tok_count, 128), 0) // SEQ_LEN
    lane = lax.broadcasted_iota(jnp.int32, (tok_count, 128), 1)
    my_mixing = jnp.where(
        core == 0, mixing[:, : EXPERTS * half_cap], mixing[:, EXPERTS * half_cap :]
    )
    meta = lax.dot_general(
        my_mixing,
        (token_seq == lane // 2).astype(f32),
        over_tokens,
        precision=lax.Precision.HIGHEST,
        preferred_element_type=f32,
    )
    meta_high = lax.reduce_precision(meta, 8, 7)
    meta = jnp.where(lane[:1] % 2 == 0, meta_high, meta - meta_high).astype(bf16)
    grad_block = jnp.concatenate([grad_block, meta], axis=1)

    def to_experts(block_rows):
        width = block_rows.shape[1]
        block_rows = block_rows.reshape(EXPERTS, half_cap, width)
        return exchange(jnp.repeat(block_rows, replicas, axis=0)).reshape(rows, width)

    token_rows = to_experts(token_block)
    grad_full = to_experts(grad_block)

    head = lax.all_gather(reward_head, TP, axis=0, tiled=True)
    head_own = jnp.sum(w_down.astype(f32) * head[None, :], axis=1)
    head_other = jnp.sum(wd_other.astype(f32) * head[None, :], axis=1)
    head_row = jnp.concatenate([head_own, head_other])[None, :]
    local_scores = jnp.sum(tokens.astype(f32) * reward_head[None, :], axis=1)
    local_rewards = jnp.sum(local_scores.reshape(seq_local, SEQ_LEN), axis=1)
    seq_total = pair_order.shape[0]
    offset = lax.axis_index(EP) * seq_local
    placed = lax.dynamic_update_slice(jnp.zeros((seq_total,), f32), local_rewards, (offset,))
    token_rows, head_row, placed = lax.optimization_barrier((token_rows, head_row, placed))

    token_pieces = gather_features(token_rows)
    grad_pieces = gather_features(grad_full[:, :block])

    slots_hid = (rows, 2 * hid)
    meta_spec = pl.BlockSpec((rows, 128), lambda k, y: (0, block // 128))
    work = rows * 2 * hid * 4 * block
    slope, silu, hidden, score = call(
        fwd_kernel,
        piece_specs(rows, block)
        + [columns(hid, block)] * 4
        + [whole((1, 2 * hid)), meta_spec],
        [whole(slots_hid)] * 3 + [whole((ep_size, 128))],
        [jax.ShapeDtypeStruct(slots_hid, f32)] * 2
        + [jax.ShapeDtypeStruct(slots_hid, bf16), jax.ShapeDtypeStruct((ep_size, 128), f32)],
        [pltpu.VMEM(slots_hid, f32)] * 2 + [pltpu.VMEM((rows, block), bf16)],
        4 * work,
        (place, *token_pieces, w_gate, wg_other, w_up, wu_other, head_row, grad_full),
    )
    placed = (placed + score[:, :seq_local].reshape(seq_total)).reshape(2, 1, seq_total // 2)
    everyone = lax.axis_size(EP_TP)
    spread = jnp.broadcast_to(placed, (2, everyone, seq_total // 2))
    spread = lax.all_to_all(spread, EP_TP, split_axis=1, concat_axis=1, tiled=True)
    rewards = jnp.sum(spread, axis=1).reshape(seq_total) / math.sqrt(SEQ_LEN)

    down_pieces = call(
        down_kernel,
        [whole(slots_hid)] + [columns(hid, block)] * 2,
        piece_specs(rows, block),
        piece_shapes(rows, block),
        [pltpu.VMEM((rows, block), bf16)],
        2 * work,
        (place, hidden, w_down, wd_other),
    )
    partial = call(
        back_kernel,
        piece_specs(rows, block) + [columns(hid, block)] * 2,
        [whole(slots_hid)],
        [jax.ShapeDtypeStruct(slots_hid, f32)],
        [pltpu.VMEM((rows, block), bf16)],
        2 * work,
        (place, *grad_pieces, w_down, wd_other),
    )[0]
    down_sums = scatter_start(down_pieces)

    seq_iota = jnp.arange(seq_total, dtype=jnp.int32)
    chosen_hot = (pair_order[0::2][:, None] == seq_iota[None, :]).astype(f32)
    rejected_hot = (pair_order[1::2][:, None] == seq_iota[None, :]).astype(f32)
    margin = jnp.sum((chosen_hot - rejected_hot) * rewards[None, :], axis=1)
    pair_loss = jnp.mean(jax.nn.softplus(-margin))
    pair_weight = jax.nn.sigmoid(-margin)
    seq_coef = jnp.sum(pair_weight[:, None] * (rejected_hot - chosen_hot), axis=0)
    token_coef = jnp.repeat(lax.dynamic_slice_in_dim(seq_coef, offset, seq_local), SEQ_LEN)
    grad_out = (
        upstream.astype(f32)
        + loss_scale * token_coef[:, None] * reward_head[None, :] / math.sqrt(SEQ_LEN)
    ).astype(bf16)
    scaled = (seq_coef * (loss_scale / math.sqrt(SEQ_LEN))).reshape(ep_size, seq_local)

    gate_grad, up_grad, slot_coef, *input_pieces = call(
        bwd_kernel,
        [columns(hid, block)] * 4
        + [whole((1, 2 * hid)), meta_spec, whole((ep_size, seq_local))]
        + [whole(slots_hid)] * 3,
        [whole(slots_hid)] * 2 + [whole((rows, 1))] + piece_specs(rows, block),
        [jax.ShapeDtypeStruct(slots_hid, bf16)] * 2
        + [jax.ShapeDtypeStruct((rows, 1), f32)]
        + piece_shapes(rows, block),
        [pltpu.VMEM((rows, block), bf16)],
        4 * work,
        (place, w_gate, wg_other, w_up, wu_other, head_row, grad_full, scaled)
        + (partial, slope, silu),
    )
    input_sums = scatter_start(input_pieces)

    *own_grads, other_grads = call(
        grad_kernel,
        piece_specs(rows, block) * 2
        + [whole(slots_hid)] * 3
        + [whole((rows, 1)), columns(1, block)],
        [columns(hid, block)] * 3 + [columns(3 * hid, block)],
        [jax.ShapeDtypeStruct((hid, 4 * block), bf16)] * 3
        + [jax.ShapeDtypeStruct((3 * hid, 4 * block), bf16)],
        [pltpu.VMEM((3, 2 * hid, rows), bf16), pltpu.VMEM((rows, block), bf16)],
        6 * work,
        (place, *token_pieces, *grad_pieces, hidden, gate_grad, up_grad, slot_coef, head[None, :]),
    )
    other_grads = swap(other_grads)
    grad_gate, grad_up, grad_down = (
        add(own, other_grads[i * hid : (i + 1) * hid]) for i, own in enumerate(own_grads)
    )

    def come_back(pieces):
        summed = add(*pieces).reshape(ep_size, half_cap, block)
        arrived = exchange(summed).astype(f32)
        sums = jnp.sum(arrived.reshape(EXPERTS, replicas, half_cap, block), axis=1)
        sums = sums.astype(bf16).reshape(EXPERTS * half_cap, block)
        left, right = sums[:, :local_width], sums[:, local_width:]
        mine = jnp.where(core == 0, left, right)
        theirs = swap(jnp.where(core == 0, right, left))
        return jnp.concatenate(
            [jnp.where(core == 0, mine, theirs), jnp.where(core == 0, theirs, mine)], axis=0
        )

    mixed_sum = plain(mixing, come_back(down_sums).astype(f32))
    layer_out = (tokens.astype(f32) + mixed_sum).astype(bf16)
    returned = plain(picker.astype(bf16), come_back(input_sums))
    grad_tokens = (grad_out.astype(f32) + returned).astype(bf16)
    return (layer_out, rewards, pair_loss, grad_tokens, grad_gate, grad_up, grad_down)


def solution(mesh):
    split = Mesh(mesh.devices.reshape(4, 8, 4, 2), EP_TP)
    in_specs = (
        P(EP, TP),
        P(EP, None),
        P(EP),
        P(EP_TP, None),
        P(EP_TP, None),
        P(EP_TP, None),
        P(TP),
        P(EP, TP),
        P(),
    )
    out_specs = (P(EP, TP), P(), P(), P(EP, TP), P(EP_TP, None), P(EP_TP, None), P(EP_TP, None))
    return jax.shard_map(layer, mesh=split, in_specs=in_specs, out_specs=out_specs, check_vma=False)
```

```python
import math

import jax
import jax.numpy as jnp
from jax import lax
from jax.experimental import pallas as pl
from jax.experimental.pallas import tpu as pltpu
from jax.sharding import Mesh
from jax.sharding import PartitionSpec as P


EXPERTS = 8
SEQ_LEN = 64
EP = ("ep_x", "ep_z")
TP = ("tp_y", "tp_c")
EP_TP = EP + TP


loss_scale = 256.0
VMEM_MIB = 60
bf16, f32 = jnp.bfloat16, jnp.float32


def route_tables(expert_ids, route_share, capacity):
    experts_iota = jnp.arange(EXPERTS, dtype=jnp.int32)
    first_hot = (expert_ids[:, 0:1] == experts_iota[None, :]).astype(jnp.int32)
    second_hot = (expert_ids[:, 1:2] == experts_iota[None, :]).astype(jnp.int32)
    first_rank = jnp.sum((jnp.cumsum(first_hot, axis=0) - first_hot) * first_hot, axis=1)
    second_before = (
        jnp.cumsum(second_hot, axis=0) - second_hot + jnp.sum(first_hot, axis=0)[None, :]
    )
    second_rank = jnp.sum(second_before * second_hot, axis=1)
    route_ranks = jnp.stack([first_rank, second_rank], axis=1)
    route_kept = route_ranks < capacity
    half = capacity // 2
    slot_index = (route_ranks // half) * (EXPERTS * half) + expert_ids * half + route_ranks % half
    slot_index = jnp.where(route_kept, slot_index, -1)
    shares = jnp.stack([route_share, 1.0 - route_share], axis=1) * route_kept.astype(f32)
    slot_iota = jnp.arange(EXPERTS * capacity, dtype=jnp.int32)
    matches = (slot_index[:, :, None] == slot_iota[None, None, :]).astype(f32)
    picker = jnp.sum(matches, axis=1)
    mixing = jnp.sum(matches * shares[:, :, None], axis=1)
    return (picker, mixing)


def rot(value, shift):
    return lax.ppermute(value, "tp_y", [(i, (i + shift) % 4) for i in range(4)])


def swap(value):
    return lax.ppermute(value, "tp_c", [(0, 1), (1, 0)])


def exchange(blocks):
    arrived = lax.all_to_all(
        blocks.transpose(1, 0, 2), EP, split_axis=1, concat_axis=1, tiled=True
    )
    return arrived.transpose(1, 0, 2)


def gather_features(rows):
    half = rows.shape[0] // 2
    back, ahead = rot(rows, 1), rot(rows, -1)
    far_low, far_high = rot(back[:half], 1), rot(ahead[half:], -1)
    return (rows, ahead, far_low, far_high, back)


def add(*terms):
    return sum((t.astype(f32) for t in terms[1:]), terms[0].astype(f32)).astype(bf16)


def scatter_start(pieces):
    own, ahead, far_low, far_high, back = pieces
    half = far_low.shape[0]
    via_low, via_high = rot(far_low, 1), rot(far_high, -1)
    onward = jnp.concatenate([add(ahead[:half], via_low), ahead[half:]], axis=0)
    backward = jnp.concatenate([back[:half], add(back[half:], via_high)], axis=0)
    return own, rot(onward, 1), rot(backward, -1)


def piece_halves(refs):
    own, ahead, far_low, far_high, back = refs
    half = far_low.shape[0]
    low, high = pl.ds(0, half), pl.ds(half, half)
    return (
        (own.at[low], own.at[high]),
        (ahead.at[low], ahead.at[high]),
        (far_low, far_high),
        (back.at[low], back.at[high]),
    )


def load_piece(step, refs, rows):
    half = rows.shape[0] // 2
    for k, (low, high) in enumerate(piece_halves(refs)):

        @pl.when(step == k)
        def _(low=low, high=high):
            rows[pl.ds(0, half)] = low[...]
            rows[pl.ds(half, half)] = high[...]


def cross(a, b):
    return lax.dot_general(a, b, (((1,), (1,)), ((), ())), preferred_element_type=f32)


def plain(a, b):
    return lax.dot_general(a, b, (((1,), (0,)), ((), ())), preferred_element_type=f32)


def near_kernel(y_ref, *refs):
    x_refs = refs[:3]
    weights, accs, rows = refs[3:7], refs[7:9], refs[9]
    width = weights[0].shape[0]
    step = pl.program_id(0)

    @pl.when(step == 0)
    def _():
        for acc in accs:
            acc[...] = jnp.zeros_like(acc)

    for k, ref in enumerate(x_refs):

        @pl.when(step == k)
        def _(ref=ref):
            rows[...] = ref[...]

    chunk = rows.shape[0] // 2

    @pl.loop(0, 2)
    def _(i):
        at = pl.ds(pl.multiple_of(i * chunk, chunk), chunk)
        for j, weight in enumerate(weights):
            accs[j // 2][at, pl.ds(j % 2 * width, width)] += cross(rows[at], weight[...])


def fwd_kernel(y_ref, *refs):
    far_refs = refs[:2]
    wg0, wg1, wu0, wu1, rh_ref, meta_ref, gate_ref, up_ref = refs[2:10]
    slope_ref, silu_ref, hidden_ref, score_ref = refs[10:14]
    gate_acc, up_acc, rows = refs[14:]
    half, width = rows.shape[0] // 2, wg0.shape[0]
    left, right = pl.ds(0, width), pl.ds(width, width)
    rows[pl.ds(0, half)] = far_refs[0][...]
    rows[pl.ds(half, half)] = far_refs[1][...]
    gate_acc[:, left] = gate_ref[:, left] + cross(rows[...], wg0[...])
    gate_acc[:, right] = gate_ref[:, right] + cross(rows[...], wg1[...])
    up_acc[:, left] = up_ref[:, left] + cross(rows[...], wu0[...])
    up_acc[:, right] = up_ref[:, right] + cross(rows[...], wu1[...])
    finish_forward(
        rh_ref, meta_ref, slope_ref, silu_ref, hidden_ref, score_ref, gate_acc, up_acc
    )


def finish_forward(
    rh_ref, meta_ref, slope_ref, silu_ref, hidden_ref, score_ref, gate_acc, up_acc
):
    chunk = gate_acc.shape[0] // 8

    @pl.loop(0, 8)
    def _(i):
        at = pl.ds(pl.multiple_of(i * chunk, chunk), chunk)
        gate, up = gate_acc[at], up_acc[at]
        sig = jax.nn.sigmoid(gate)
        silu = gate * sig
        hidden = (silu * up).astype(bf16)
        silu_ref[at] = silu
        slope_ref[at] = up * (sig * (1.0 + gate * (1.0 - sig)))
        hidden_ref[at] = hidden
        score = jnp.sum(hidden.astype(f32) * rh_ref[...], axis=1, keepdims=True)
        gate_acc[at, pl.ds(0, 128)] = score * meta_ref[at].astype(f32)

    scores = gate_acc[:, pl.ds(0, 128)].reshape(score_ref.shape[0], -1, 128)
    scores = jnp.sum(scores, axis=1)
    lane = lax.broadcasted_iota(jnp.int32, scores.shape, 1)
    first = jnp.sum(jnp.where(lane < 2, scores, 0.0), axis=1, keepdims=True)
    second = jnp.sum(jnp.where(lane < 2, 0.0, scores), axis=1, keepdims=True)
    score_ref[...] = jnp.where(lane == 0, first, second)


def down_kernel(y_ref, hidden_ref, wd0, wd1, low_ref, high_ref):
    width, half = wd0.shape[0], low_ref.shape[0]
    left, right = pl.ds(0, width), pl.ds(width, width)
    for i, ref in enumerate((low_ref, high_ref)):
        at = pl.ds(i * half, half)
        ref[...] = (
            plain(hidden_ref[at, left], wd0[...]) + plain(hidden_ref[at, right], wd1[...])
        ).astype(bf16)


def side_kernel(y_ref, hidden_ref, wd0, wd1, *refs):
    out_refs, rows = refs[:3], refs[3]
    width = wd0.shape[0]
    left, right = pl.ds(0, width), pl.ds(width, width)
    chunk = rows.shape[0] // 2

    @pl.loop(0, 2)
    def _(i):
        at = pl.ds(pl.multiple_of(i * chunk, chunk), chunk)
        rows[at] = (
            plain(hidden_ref[at, left], wd0[...]) + plain(hidden_ref[at, right], wd1[...])
        ).astype(bf16)

    for k, ref in enumerate(out_refs):

        @pl.when(pl.program_id(0) == k)
        def _(ref=ref):
            ref[...] = rows[...]


def back_kernel(y_ref, *refs):
    u_refs, (wd0, wd1, out_ref, rows) = refs[:5], refs[5:]
    width = wd0.shape[0]
    left, right = pl.ds(0, width), pl.ds(width, width)
    step = pl.program_id(0)

    @pl.when(step == 0)
    def _():
        out_ref[...] = jnp.zeros_like(out_ref)

    load_piece(step, u_refs, rows)
    out_ref[:, left] += cross(rows[...], wd0[...])
    out_ref[:, right] += cross(rows[...], wd1[...])


def bwd_kernel(y_ref, *refs):
    wg0, wg1, wu0, wu1, rh_ref, meta_ref, seq_ref, partial_ref, slope_ref, silu_ref = refs[:10]
    gate_grad_ref, up_grad_ref, coef_ref, low_ref, high_ref = refs[10:15]
    width, half = wg0.shape[0], low_ref.shape[0]
    left, right = pl.ds(0, width), pl.ds(width, width)
    count = partial_ref.shape[0]
    blocks = seq_ref.shape[0]
    lane = lax.broadcasted_iota(jnp.int32, (blocks, 128), 1)
    first = jnp.broadcast_to(seq_ref[:, pl.ds(0, 1)], lane.shape)
    second = jnp.broadcast_to(seq_ref[:, pl.ds(1, 1)], lane.shape)
    by_lane = jnp.where(lane < 2, first, jnp.where(lane < 4, second, 0.0))
    shares = meta_ref[...].astype(f32).reshape(blocks, count // blocks, 128)
    terms = (shares * by_lane[:, None, :]).reshape(count, 128)
    coef_ref[...] = jnp.sum(terms, axis=1, keepdims=True)
    chunk = count // 8

    @pl.loop(0, 8)
    def _(i):
        at = pl.ds(pl.multiple_of(i * chunk, chunk), chunk)
        hidden_grad = partial_ref[at] + coef_ref[at] * rh_ref[...]
        gate_grad_ref[at] = (hidden_grad * slope_ref[at]).astype(bf16)
        up_grad_ref[at] = (hidden_grad * silu_ref[at]).astype(bf16)

    for i, ref in enumerate((low_ref, high_ref)):
        at = pl.ds(i * half, half)
        ref[...] = (
            plain(gate_grad_ref[at, left], wg0[...])
            + plain(gate_grad_ref[at, right], wg1[...])
            + plain(up_grad_ref[at, left], wu0[...])
            + plain(up_grad_ref[at, right], wu1[...])
        ).astype(bf16)


def rest_kernel(y_ref, *refs):
    wg0, wg1, wu0, wu1, gate_grad_ref, up_grad_ref = refs[:6]
    out_refs, rows = refs[6:9], refs[9]
    width = wg0.shape[0]
    left, right = pl.ds(0, width), pl.ds(width, width)
    chunk = rows.shape[0] // 2

    @pl.loop(0, 2)
    def _(i):
        at = pl.ds(pl.multiple_of(i * chunk, chunk), chunk)
        rows[at] = (
            plain(gate_grad_ref[at, left], wg0[...])
            + plain(gate_grad_ref[at, right], wg1[...])
            + plain(up_grad_ref[at, left], wu0[...])
            + plain(up_grad_ref[at, right], wu1[...])
        ).astype(bf16)

    for k, ref in enumerate(out_refs):

        @pl.when(pl.program_id(0) == k)
        def _(ref=ref):
            ref[...] = rows[...]


def grad_kernel(y_ref, *refs):
    x_refs, u_refs = refs[:5], refs[5:10]
    hidden_ref, gate_grad_ref, up_grad_ref, coef_ref, rh_ref = refs[10:15]
    own_ref, other_ref, left, rows = refs[15:]
    width = left.shape[1]
    step = pl.program_id(0)

    @pl.when(step == 0)
    def _():
        for i, ref in enumerate((gate_grad_ref, up_grad_ref, hidden_ref)):
            turned = ref[...].T
            left[2 * i] = turned[:width]
            left[2 * i + 1] = turned[width:]

    load_piece(step, x_refs, rows.at[0])
    load_piece(step, u_refs, rows.at[1])
    rows[1] = (rows[1].astype(f32) + coef_ref[...] * rh_ref[...]).astype(bf16)

    @pl.loop(0, 3)
    def _(i):
        at = pl.ds(pl.multiple_of(i * width, width), width)
        own_ref[at] = plain(left[2 * i], rows[i // 2]).astype(bf16)
        other_ref[at] = plain(left[2 * i + 1], rows[i // 2]).astype(bf16)


def whole(shape):
    return pl.BlockSpec(shape, lambda k, y: (0,) * len(shape))


def columns(width, block):
    return pl.BlockSpec((width, block), lambda k, y: (0, (y[0] + k) % 4))


def near_columns(width, block):
    return pl.BlockSpec((width, block), lambda k, y: (0, (y[0] + k + k // 2) % 4))


def far_columns(width, block):
    return pl.BlockSpec((width, block), lambda k, y: (0, (y[0] + 2) % 4))


def piece_specs(rows, block):
    full, part = whole((rows, block)), whole((rows // 2, block))
    return [full, full, part, part, full]


def call(kernel, steps, in_specs, out_specs, out_shape, scratch, flops, args):
    return pl.pallas_call(
        kernel,
        grid_spec=pltpu.PrefetchScalarGridSpec(
            num_scalar_prefetch=1,
            grid=(steps,),
            in_specs=in_specs,
            out_specs=out_specs,
            scratch_shapes=scratch,
        ),
        out_shape=out_shape,
        compiler_params=pltpu.CompilerParams(
            dimension_semantics=("arbitrary",), vmem_limit_bytes=VMEM_MIB * 1024 * 1024
        ),
        cost_estimate=pl.CostEstimate(flops=flops, bytes_accessed=20_000_000, transcendentals=0),
    )(*args)


def layer(
    tokens, expert_ids, route_share, w_gate, w_up, w_down, reward_head, upstream, pair_order
):
    tok_count, local_width = tokens.shape
    capacity = tok_count * expert_ids.shape[1] // EXPERTS
    ep_size = lax.axis_size(EP)
    replicas = ep_size // EXPERTS
    half_cap = capacity // 2
    block = 2 * local_width
    rows = ep_size * half_cap
    hid = w_gate.shape[0]
    core = lax.axis_index("tp_c")
    place = lax.axis_index("tp_y").astype(jnp.int32).reshape(1)

    wg_other, wu_other, wd_other = swap(w_gate), swap(w_up), swap(w_down)

    picker, mixing = route_tables(expert_ids, route_share, capacity)
    seq_local = tok_count // SEQ_LEN
    over_tokens = (((0,), (0,)), ((), ()))
    both = lax.dot_general(
        picker.astype(bf16),
        jnp.concatenate([tokens, upstream], axis=1),
        over_tokens,
        preferred_element_type=f32,
    )
    slot_share = jnp.sum(mixing, axis=0)
    column = lax.broadcasted_iota(jnp.int32, (1, 2 * local_width), 1)
    both = both * jnp.where(column < local_width, 1.0, slot_share[:, None])
    both = both.astype(bf16).reshape(2, EXPERTS * half_cap, 2 * local_width)
    mine = lax.dynamic_index_in_dim(both, core, 0, keepdims=False)
    theirs = swap(lax.dynamic_index_in_dim(both, 1 - core, 0, keepdims=False))
    low = jnp.where(core == 0, mine, theirs)
    high = jnp.where(core == 0, theirs, mine)
    token_block = jnp.concatenate([low[:, :local_width], high[:, :local_width]], axis=1)
    grad_block = jnp.concatenate([low[:, local_width:], high[:, local_width:]], axis=1)

    token_seq = lax.broadcasted_iota(jnp.int32, (tok_count, 128), 0) // SEQ_LEN
    lane = lax.broadcasted_iota(jnp.int32, (tok_count, 128), 1)
    my_mixing = jnp.where(
        core == 0, mixing[:, : EXPERTS * half_cap], mixing[:, EXPERTS * half_cap :]
    )
    meta = lax.dot_general(
        my_mixing,
        (token_seq == lane // 2).astype(f32),
        over_tokens,
        precision=lax.Precision.HIGHEST,
        preferred_element_type=f32,
    )
    meta_high = lax.reduce_precision(meta, 8, 7)
    meta = jnp.where(lane[:1] % 2 == 0, meta_high, meta - meta_high).astype(bf16)
    grad_block = jnp.concatenate([grad_block, meta], axis=1)

    def to_experts(block_rows):
        width = block_rows.shape[1]
        block_rows = block_rows.reshape(EXPERTS, half_cap, width)
        return exchange(jnp.repeat(block_rows, replicas, axis=0)).reshape(rows, width)

    token_rows = to_experts(token_block)
    grad_full = to_experts(grad_block)

    head = lax.all_gather(reward_head, TP, axis=0, tiled=True)
    head_own = jnp.sum(w_down.astype(f32) * head[None, :], axis=1)
    head_other = jnp.sum(wd_other.astype(f32) * head[None, :], axis=1)
    head_row = jnp.concatenate([head_own, head_other])[None, :]
    local_scores = jnp.sum(tokens.astype(f32) * reward_head[None, :], axis=1)
    local_rewards = jnp.sum(local_scores.reshape(seq_local, SEQ_LEN), axis=1)
    seq_total = pair_order.shape[0]
    offset = lax.axis_index(EP) * seq_local
    placed = lax.dynamic_update_slice(jnp.zeros((seq_total,), f32), local_rewards, (offset,))
    token_rows, head_row, placed = lax.optimization_barrier((token_rows, head_row, placed))

    token_pieces = gather_features(token_rows)
    grad_pieces = gather_features(grad_full[:, :block])

    slots_hid = (rows, 2 * hid)
    meta_spec = pl.BlockSpec((rows, 128), lambda k, y: (0, block // 128))
    work = rows * 2 * hid * 4 * block
    own_rows, ahead_rows, far_low, far_high, back_rows = token_pieces
    gate_weights = (w_gate, wg_other, w_up, wu_other)
    full, part = whole((rows, block)), whole((rows // 2, block))
    gate, up = call(
        near_kernel,
        3,
        [full] * 3 + [near_columns(hid, block)] * 4,
        [whole(slots_hid)] * 2,
        [jax.ShapeDtypeStruct(slots_hid, f32)] * 2,
        [pltpu.VMEM((rows, block), bf16)],
        3 * work,
        (place, own_rows, ahead_rows, back_rows, *gate_weights),
    )
    slope, silu, hidden, score = call(
        fwd_kernel,
        1,
        [part] * 2
        + [far_columns(hid, block)] * 4
        + [whole((1, 2 * hid)), meta_spec]
        + [whole(slots_hid)] * 2,
        [whole(slots_hid)] * 3 + [whole((ep_size, 128))],
        [jax.ShapeDtypeStruct(slots_hid, f32)] * 2
        + [jax.ShapeDtypeStruct(slots_hid, bf16), jax.ShapeDtypeStruct((ep_size, 128), f32)],
        [pltpu.VMEM(slots_hid, f32)] * 2 + [pltpu.VMEM((rows, block), bf16)],
        work,
        (place, far_low, far_high, *gate_weights, head_row, grad_full, gate, up),
    )
    placed = (placed + score[:, :seq_local].reshape(seq_total)).reshape(2, 1, seq_total // 2)
    everyone = lax.axis_size(EP_TP)
    spread = jnp.broadcast_to(placed, (2, everyone, seq_total // 2))
    spread = lax.all_to_all(spread, EP_TP, split_axis=1, concat_axis=1, tiled=True)
    rewards = jnp.sum(spread, axis=1).reshape(seq_total) / math.sqrt(SEQ_LEN)

    half_shape = jax.ShapeDtypeStruct((rows // 2, block), bf16)
    full_shape = jax.ShapeDtypeStruct((rows, block), bf16)
    down_low, down_high = call(
        down_kernel,
        1,
        [whole(slots_hid)] + [far_columns(hid, block)] * 2,
        [part] * 2,
        [half_shape] * 2,
        [],
        work // 2,
        (place, hidden, w_down, wd_other),
    )
    down_own, down_ahead, down_back = call(
        side_kernel,
        3,
        [whole(slots_hid)] + [near_columns(hid, block)] * 2,
        [full] * 3,
        [full_shape] * 3,
        [pltpu.VMEM((rows, block), bf16)],
        3 * work // 2,
        (place, hidden, w_down, wd_other),
    )
    down_pieces = (down_own, down_ahead, down_low, down_high, down_back)
    partial = call(
        back_kernel,
        4,
        piece_specs(rows, block) + [columns(hid, block)] * 2,
        [whole(slots_hid)],
        [jax.ShapeDtypeStruct(slots_hid, f32)],
        [pltpu.VMEM((rows, block), bf16)],
        2 * work,
        (place, *grad_pieces, w_down, wd_other),
    )[0]
    down_sums = scatter_start(down_pieces)

    seq_iota = jnp.arange(seq_total, dtype=jnp.int32)
    chosen_hot = (pair_order[0::2][:, None] == seq_iota[None, :]).astype(f32)
    rejected_hot = (pair_order[1::2][:, None] == seq_iota[None, :]).astype(f32)
    margin = jnp.sum((chosen_hot - rejected_hot) * rewards[None, :], axis=1)
    pair_loss = jnp.mean(jax.nn.softplus(-margin))
    pair_weight = jax.nn.sigmoid(-margin)
    seq_coef = jnp.sum(pair_weight[:, None] * (rejected_hot - chosen_hot), axis=0)
    token_coef = jnp.repeat(lax.dynamic_slice_in_dim(seq_coef, offset, seq_local), SEQ_LEN)
    grad_out = (
        upstream.astype(f32)
        + loss_scale * token_coef[:, None] * reward_head[None, :] / math.sqrt(SEQ_LEN)
    ).astype(bf16)
    scaled = (seq_coef * (loss_scale / math.sqrt(SEQ_LEN))).reshape(ep_size, seq_local)

    gate_grad, up_grad, slot_coef, far_low, far_high = call(
        bwd_kernel,
        1,
        [far_columns(hid, block)] * 4
        + [whole((1, 2 * hid)), meta_spec, whole((ep_size, seq_local))]
        + [whole(slots_hid)] * 3,
        [whole(slots_hid)] * 2 + [whole((rows, 1))] + [part] * 2,
        [jax.ShapeDtypeStruct(slots_hid, bf16)] * 2
        + [jax.ShapeDtypeStruct((rows, 1), f32)]
        + [jax.ShapeDtypeStruct((rows // 2, block), bf16)] * 2,
        [],
        work,
        (place, *gate_weights, head_row, grad_full, scaled, partial, slope, silu),
    )
    own_sums, ahead_sums, back_sums = call(
        rest_kernel,
        3,
        [near_columns(hid, block)] * 4 + [whole(slots_hid)] * 2,
        [full] * 3,
        [jax.ShapeDtypeStruct((rows, block), bf16)] * 3,
        [pltpu.VMEM((rows, block), bf16)],
        3 * work,
        (place, *gate_weights, gate_grad, up_grad),
    )
    input_sums = scatter_start((own_sums, ahead_sums, far_low, far_high, back_sums))

    own_grads, other_grads = call(
        grad_kernel,
        4,
        piece_specs(rows, block) * 2
        + [whole(slots_hid)] * 3
        + [whole((rows, 1)), columns(1, block)],
        [columns(3 * hid, block)] * 2,
        [jax.ShapeDtypeStruct((3 * hid, 4 * block), bf16)] * 2,
        [pltpu.VMEM((6, hid, rows), bf16), pltpu.VMEM((2, rows, block), bf16)],
        6 * work,
        (place, *token_pieces, *grad_pieces, hidden, gate_grad, up_grad, slot_coef, head[None, :]),
    )
    other_grads = swap(other_grads)
    grad_gate, grad_up, grad_down = (
        add(own_grads[i * hid : (i + 1) * hid], other_grads[i * hid : (i + 1) * hid])
        for i in range(3)
    )

    def come_back(pieces):
        summed = add(*pieces).reshape(ep_size, half_cap, block)
        arrived = exchange(summed).astype(f32)
        sums = jnp.sum(arrived.reshape(EXPERTS, replicas, half_cap, block), axis=1)
        sums = sums.astype(bf16).reshape(EXPERTS * half_cap, block)
        left, right = sums[:, :local_width], sums[:, local_width:]
        mine = jnp.where(core == 0, left, right)
        theirs = swap(jnp.where(core == 0, right, left))
        return jnp.concatenate(
            [jnp.where(core == 0, mine, theirs), jnp.where(core == 0, theirs, mine)], axis=0
        )

    mixed_sum = plain(mixing, come_back(down_sums).astype(f32))
    layer_out = (tokens.astype(f32) + mixed_sum).astype(bf16)
    returned = plain(picker.astype(bf16), come_back(input_sums))
    grad_tokens = (grad_out.astype(f32) + returned).astype(bf16)
    return (layer_out, rewards, pair_loss, grad_tokens, grad_gate, grad_up, grad_down)


def solution(mesh):
    split = Mesh(mesh.devices.reshape(4, 8, 4, 2), EP_TP)
    in_specs = (
        P(EP, TP),
        P(EP, None),
        P(EP),
        P(EP_TP, None),
        P(EP_TP, None),
        P(EP_TP, None),
        P(TP),
        P(EP, TP),
        P(),
    )
    out_specs = (P(EP, TP), P(), P(), P(EP, TP), P(EP_TP, None), P(EP_TP, None), P(EP_TP, None))
    return jax.shard_map(layer, mesh=split, in_specs=in_specs, out_specs=out_specs, check_vma=False)
```

```python
import math

import jax
import jax.numpy as jnp
from jax import lax
from jax.experimental import pallas as pl
from jax.experimental.pallas import tpu as pltpu
from jax.sharding import Mesh
from jax.sharding import PartitionSpec as P


EXPERTS = 8
SEQ_LEN = 64
EP = ("ep_x", "ep_z")
TP = ("tp_y", "tp_c")
EP_TP = EP + TP


loss_scale = 256.0
VMEM_MIB = 60
bf16, f32 = jnp.bfloat16, jnp.float32


def route_kernel(at_ref, ids_ref, share_ref, tokens_ref, upstream_ref, *refs):
    mine_ref, theirs_ref, meta_ref, picker_ref, mixing_ref, both, meta = refs
    count, slots = picker_ref.shape
    local_width = tokens_ref.shape[1]
    half_cap = slots // (2 * EXPERTS)
    lane = lax.broadcasted_iota(jnp.int32, (count, count), 1)
    row = lax.broadcasted_iota(jnp.int32, (count, count), 0)
    earlier = (lane < row).astype(f32)
    hot = [(lane == ids_ref[:, pl.ds(i, 1)]).astype(f32) for i in (0, 1)]
    before = [plain(earlier.astype(bf16), h.astype(bf16)) for h in hot]
    before[1] = before[1] + jnp.sum(hot[0], axis=0, keepdims=True)
    slot_iota = lax.broadcasted_iota(jnp.int32, (count, slots), 1)
    share = share_ref[...]
    picker = jnp.zeros((count, slots), f32)
    mixing = jnp.zeros((count, slots), f32)
    for i, weight in ((0, share), (1, 1.0 - share)):
        rank = jnp.sum(before[i] * hot[i], axis=1, keepdims=True).astype(jnp.int32)
        late = (rank >= half_cap).astype(jnp.int32)
        slot = late * (slots // 2 - half_cap) + ids_ref[:, pl.ds(i, 1)] * half_cap + rank
        slot = jnp.where(rank < 2 * half_cap, slot, -1)
        match = (slot_iota == slot).astype(f32)
        picker = picker + match
        mixing = mixing + match * weight
    picker_ref[...] = picker.astype(bf16)
    mixing_ref[...] = mixing
    by_slot = picker.T.astype(bf16)
    shares = mixing.T
    slot_share = jnp.sum(shares, axis=1, keepdims=True)
    both[:, pl.ds(0, local_width)] = plain(by_slot, tokens_ref[...]).astype(bf16)
    both[:, pl.ds(local_width, local_width)] = (
        plain(by_slot, upstream_ref[...]) * slot_share
    ).astype(bf16)
    lane = lax.broadcasted_iota(jnp.int32, (slots, count), 1)
    table = jnp.zeros((slots, count), f32)
    for seq in range(count // SEQ_LEN):
        part = jnp.where(lane // SEQ_LEN == seq, shares, 0.0)
        part = jnp.sum(part, axis=1, keepdims=True)
        high = part.astype(bf16).astype(f32)
        table = jnp.where(lane == 2 * seq, high, table)
        table = jnp.where(lane == 2 * seq + 1, part - high, table)
    meta[...] = table.astype(bf16)
    half = slots // 2
    core = at_ref[1]
    own = pl.ds(pl.multiple_of(core * half, half), half)
    other = pl.ds(pl.multiple_of((1 - core) * half, half), half)
    mine_ref[...] = both[own]
    theirs_ref[...] = both[other]
    meta_ref[...] = meta[own]


def pack_kernel(at_ref, mine_ref, got_ref, meta_ref, token_ref, grad_ref):
    local_width = mine_ref.shape[1] // 2
    half_cap = mine_ref.shape[0] // EXPERTS
    replicas = token_ref.shape[0] // mine_ref.shape[0]
    for core in (0, 1):
        low, high = (mine_ref, got_ref) if core == 0 else (got_ref, mine_ref)

        @pl.when(at_ref[1] == core)
        def _(low=low, high=high):
            for i in range(EXPERTS * replicas):
                src = pl.ds(i // replicas * half_cap, half_cap)
                dst = pl.ds(i * half_cap, half_cap)
                token_ref[dst, pl.ds(0, local_width)] = low[src, pl.ds(0, local_width)]
                token_ref[dst, pl.ds(local_width, local_width)] = high[src, pl.ds(0, local_width)]
                grad_ref[dst, pl.ds(0, local_width)] = low[src, pl.ds(local_width, local_width)]
                grad_ref[dst, pl.ds(local_width, local_width)] = high[
                    src, pl.ds(local_width, local_width)
                ]
                token_ref[dst, pl.ds(2 * local_width, 128)] = meta_ref[src]


def rot(value, shift):
    return lax.ppermute(value, "tp_y", [(i, (i + shift) % 4) for i in range(4)])


def swap(value):
    return lax.ppermute(value, "tp_c", [(0, 1), (1, 0)])


def exchange(blocks):
    arrived = lax.all_to_all(
        blocks.transpose(1, 0, 2), EP, split_axis=1, concat_axis=1, tiled=True
    )
    return arrived.transpose(1, 0, 2)


def gather_features(rows):
    half = rows.shape[0] // 2
    back, ahead = rot(rows, 1), rot(rows, -1)
    far_low, far_high = rot(back[:half], 1), rot(ahead[half:], -1)
    return (rows, ahead, far_low, far_high, back)


def add(*terms):
    return sum((t.astype(f32) for t in terms[1:]), terms[0].astype(f32)).astype(bf16)


def scatter_start(pieces):
    own, ahead, far_low, far_high, back = pieces
    half = far_low.shape[0]
    via_low, via_high = rot(far_low, 1), rot(far_high, -1)
    onward = jnp.concatenate([add(ahead[:half], via_low), ahead[half:]], axis=0)
    backward = jnp.concatenate([back[:half], add(back[half:], via_high)], axis=0)
    return own, rot(onward, 1), rot(backward, -1)


def piece_halves(refs):
    own, ahead, far_low, far_high, back = refs
    half = far_low.shape[0]
    low, high = pl.ds(0, half), pl.ds(half, half)
    return (
        (own.at[low], own.at[high]),
        (ahead.at[low], ahead.at[high]),
        (far_low, far_high),
        (back.at[low], back.at[high]),
    )


def load_piece(step, refs, rows):
    half = rows.shape[0] // 2
    for k, (low, high) in enumerate(piece_halves(refs)):

        @pl.when(step == k)
        def _(low=low, high=high):
            rows[pl.ds(0, half)] = low[...]
            rows[pl.ds(half, half)] = high[...]


def cross(a, b):
    return lax.dot_general(a, b, (((1,), (1,)), ((), ())), preferred_element_type=f32)


def plain(a, b):
    return lax.dot_general(a, b, (((1,), (0,)), ((), ())), preferred_element_type=f32)


def near_kernel(y_ref, *refs):
    x_refs = refs[:3]
    weights, accs, rows = refs[3:7], refs[7:9], refs[9]
    width = weights[0].shape[0]
    step = pl.program_id(0)

    @pl.when(step == 0)
    def _():
        for acc in accs:
            acc[...] = jnp.zeros_like(acc)

    for k, ref in enumerate(x_refs):

        @pl.when(step == k)
        def _(ref=ref):
            rows[...] = ref[...]

    chunk = rows.shape[0] // 2

    @pl.loop(0, 2)
    def _(i):
        at = pl.ds(pl.multiple_of(i * chunk, chunk), chunk)
        for j, weight in enumerate(weights):
            accs[j // 2][at, pl.ds(j % 2 * width, width)] += cross(rows[at], weight[...])


def fwd_kernel(y_ref, *refs):
    far_refs = refs[:2]
    wg0, wg1, wu0, wu1, rh_ref, meta_ref, gate_ref, up_ref = refs[2:10]
    slope_ref, silu_ref, hidden_ref, score_ref = refs[10:14]
    gate_acc, up_acc, rows = refs[14:]
    half, width = rows.shape[0] // 2, wg0.shape[0]
    left, right = pl.ds(0, width), pl.ds(width, width)
    rows[pl.ds(0, half)] = far_refs[0][...]
    rows[pl.ds(half, half)] = far_refs[1][...]
    gate_acc[:, left] = gate_ref[:, left] + cross(rows[...], wg0[...])
    gate_acc[:, right] = gate_ref[:, right] + cross(rows[...], wg1[...])
    up_acc[:, left] = up_ref[:, left] + cross(rows[...], wu0[...])
    up_acc[:, right] = up_ref[:, right] + cross(rows[...], wu1[...])
    finish_forward(
        rh_ref, meta_ref, slope_ref, silu_ref, hidden_ref, score_ref, gate_acc, up_acc
    )


def finish_forward(
    rh_ref, meta_ref, slope_ref, silu_ref, hidden_ref, score_ref, gate_acc, up_acc
):
    chunk = gate_acc.shape[0] // 8

    @pl.loop(0, 8)
    def _(i):
        at = pl.ds(pl.multiple_of(i * chunk, chunk), chunk)
        gate, up = gate_acc[at], up_acc[at]
        sig = jax.nn.sigmoid(gate)
        silu = gate * sig
        hidden = (silu * up).astype(bf16)
        silu_ref[at] = silu
        slope_ref[at] = up * (sig * (1.0 + gate * (1.0 - sig)))
        hidden_ref[at] = hidden
        score = jnp.sum(hidden.astype(f32) * rh_ref[...], axis=1, keepdims=True)
        gate_acc[at, pl.ds(0, 128)] = score * meta_ref[at].astype(f32)

    scores = gate_acc[:, pl.ds(0, 128)].reshape(score_ref.shape[0], -1, 128)
    scores = jnp.sum(scores, axis=1)
    lane = lax.broadcasted_iota(jnp.int32, scores.shape, 1)
    first = jnp.sum(jnp.where(lane < 2, scores, 0.0), axis=1, keepdims=True)
    second = jnp.sum(jnp.where(lane < 2, 0.0, scores), axis=1, keepdims=True)
    score_ref[...] = jnp.where(lane == 0, first, second)


def down_kernel(y_ref, hidden_ref, wd0, wd1, low_ref, high_ref):
    width, half = wd0.shape[0], low_ref.shape[0]
    left, right = pl.ds(0, width), pl.ds(width, width)
    for i, ref in enumerate((low_ref, high_ref)):
        at = pl.ds(i * half, half)
        ref[...] = (
            plain(hidden_ref[at, left], wd0[...]) + plain(hidden_ref[at, right], wd1[...])
        ).astype(bf16)


def side_kernel(y_ref, hidden_ref, wd0, wd1, *refs):
    out_refs, rows = refs[:3], refs[3]
    width = wd0.shape[0]
    left, right = pl.ds(0, width), pl.ds(width, width)
    chunk = rows.shape[0] // 2

    @pl.loop(0, 2)
    def _(i):
        at = pl.ds(pl.multiple_of(i * chunk, chunk), chunk)
        rows[at] = (
            plain(hidden_ref[at, left], wd0[...]) + plain(hidden_ref[at, right], wd1[...])
        ).astype(bf16)

    for k, ref in enumerate(out_refs):

        @pl.when(pl.program_id(0) == k)
        def _(ref=ref):
            ref[...] = rows[...]


def back_kernel(y_ref, *refs):
    u_refs, (wd0, wd1, out_ref, rows) = refs[:5], refs[5:]
    width = wd0.shape[0]
    left, right = pl.ds(0, width), pl.ds(width, width)
    step = pl.program_id(0)

    @pl.when(step == 0)
    def _():
        out_ref[...] = jnp.zeros_like(out_ref)

    load_piece(step, u_refs, rows)
    out_ref[:, left] += cross(rows[...], wd0[...])
    out_ref[:, right] += cross(rows[...], wd1[...])


def bwd_kernel(y_ref, *refs):
    wg0, wg1, wu0, wu1, rh_ref, meta_ref, seq_ref, partial_ref, slope_ref, silu_ref = refs[:10]
    gate_grad_ref, up_grad_ref, coef_ref, low_ref, high_ref = refs[10:15]
    width, half = wg0.shape[0], low_ref.shape[0]
    left, right = pl.ds(0, width), pl.ds(width, width)
    count = partial_ref.shape[0]
    blocks = seq_ref.shape[0]
    lane = lax.broadcasted_iota(jnp.int32, (blocks, 128), 1)
    first = jnp.broadcast_to(seq_ref[:, pl.ds(0, 1)], lane.shape)
    second = jnp.broadcast_to(seq_ref[:, pl.ds(1, 1)], lane.shape)
    by_lane = jnp.where(lane < 2, first, jnp.where(lane < 4, second, 0.0))
    shares = meta_ref[...].astype(f32).reshape(blocks, count // blocks, 128)
    terms = (shares * by_lane[:, None, :]).reshape(count, 128)
    coef_ref[...] = jnp.sum(terms, axis=1, keepdims=True)
    chunk = count // 8

    @pl.loop(0, 8)
    def _(i):
        at = pl.ds(pl.multiple_of(i * chunk, chunk), chunk)
        hidden_grad = partial_ref[at] + coef_ref[at] * rh_ref[...]
        gate_grad_ref[at] = (hidden_grad * slope_ref[at]).astype(bf16)
        up_grad_ref[at] = (hidden_grad * silu_ref[at]).astype(bf16)

    for i, ref in enumerate((low_ref, high_ref)):
        at = pl.ds(i * half, half)
        ref[...] = (
            plain(gate_grad_ref[at, left], wg0[...])
            + plain(gate_grad_ref[at, right], wg1[...])
            + plain(up_grad_ref[at, left], wu0[...])
            + plain(up_grad_ref[at, right], wu1[...])
        ).astype(bf16)


def rest_kernel(y_ref, *refs):
    wg0, wg1, wu0, wu1, gate_grad_ref, up_grad_ref = refs[:6]
    out_refs, rows = refs[6:9], refs[9]
    width = wg0.shape[0]
    left, right = pl.ds(0, width), pl.ds(width, width)
    chunk = rows.shape[0] // 2

    @pl.loop(0, 2)
    def _(i):
        at = pl.ds(pl.multiple_of(i * chunk, chunk), chunk)
        rows[at] = (
            plain(gate_grad_ref[at, left], wg0[...])
            + plain(gate_grad_ref[at, right], wg1[...])
            + plain(up_grad_ref[at, left], wu0[...])
            + plain(up_grad_ref[at, right], wu1[...])
        ).astype(bf16)

    for k, ref in enumerate(out_refs):

        @pl.when(pl.program_id(0) == k)
        def _(ref=ref):
            ref[...] = rows[...]


def grad_kernel(y_ref, *refs):
    x_refs, u_refs = refs[:5], refs[5:10]
    hidden_ref, gate_grad_ref, up_grad_ref, coef_ref, rh_ref = refs[10:15]
    own_ref, other_ref, left, rows = refs[15:]
    width = left.shape[1]
    step = pl.program_id(0)

    @pl.when(step == 0)
    def _():
        for i, ref in enumerate((gate_grad_ref, up_grad_ref, hidden_ref)):
            turned = ref[...].T
            left[2 * i] = turned[:width]
            left[2 * i + 1] = turned[width:]

    load_piece(step, x_refs, rows.at[0])
    load_piece(step, u_refs, rows.at[1])
    rows[1] = (rows[1].astype(f32) + coef_ref[...] * rh_ref[...]).astype(bf16)

    @pl.loop(0, 3)
    def _(i):
        at = pl.ds(pl.multiple_of(i * width, width), width)
        own_ref[at] = plain(left[2 * i], rows[i // 2]).astype(bf16)
        other_ref[at] = plain(left[2 * i + 1], rows[i // 2]).astype(bf16)


def whole(shape):
    return pl.BlockSpec(shape, lambda k, y: (0,) * len(shape))


def columns(width, block):
    return pl.BlockSpec((width, block), lambda k, y: (0, (y[0] + k) % 4))


def near_columns(width, block):
    return pl.BlockSpec((width, block), lambda k, y: (0, (y[0] + k + k // 2) % 4))


def far_columns(width, block):
    return pl.BlockSpec((width, block), lambda k, y: (0, (y[0] + 2) % 4))


def piece_specs(rows, block):
    full, part = whole((rows, block)), whole((rows // 2, block))
    return [full, full, part, part, full]


def call(kernel, steps, in_specs, out_specs, out_shape, scratch, flops, args):
    return pl.pallas_call(
        kernel,
        grid_spec=pltpu.PrefetchScalarGridSpec(
            num_scalar_prefetch=1,
            grid=(steps,),
            in_specs=in_specs,
            out_specs=out_specs,
            scratch_shapes=scratch,
        ),
        out_shape=out_shape,
        compiler_params=pltpu.CompilerParams(
            dimension_semantics=("arbitrary",), vmem_limit_bytes=VMEM_MIB * 1024 * 1024
        ),
        cost_estimate=pl.CostEstimate(flops=flops, bytes_accessed=20_000_000, transcendentals=0),
    )(*args)


def layer(
    tokens, expert_ids, route_share, w_gate, w_up, w_down, reward_head, upstream, pair_order
):
    tok_count, local_width = tokens.shape
    capacity = tok_count * expert_ids.shape[1] // EXPERTS
    ep_size = lax.axis_size(EP)
    replicas = ep_size // EXPERTS
    half_cap = capacity // 2
    block = 2 * local_width
    rows = ep_size * half_cap
    hid = w_gate.shape[0]
    core = lax.axis_index("tp_c")
    place = jnp.stack([lax.axis_index("tp_y"), core]).astype(jnp.int32)

    wg_other, wu_other, wd_other = swap(w_gate), swap(w_up), swap(w_down)

    seq_local = tok_count // SEQ_LEN
    half_slots = EXPERTS * half_cap
    half_rows = jax.ShapeDtypeStruct((half_slots, block), bf16)
    mine, theirs, meta, picker, mixing = call(
        route_kernel,
        1,
        [whole((tok_count, 2)), whole((tok_count, 1))] + [whole((tok_count, local_width))] * 2,
        [whole((half_slots, block))] * 2
        + [whole((half_slots, 128))]
        + [whole((tok_count, 2 * half_slots))] * 2,
        [
            half_rows,
            half_rows,
            jax.ShapeDtypeStruct((half_slots, 128), bf16),
            jax.ShapeDtypeStruct((tok_count, 2 * half_slots), bf16),
            jax.ShapeDtypeStruct((tok_count, 2 * half_slots), f32),
        ],
        [
            pltpu.VMEM((2 * half_slots, block), bf16),
            pltpu.VMEM((2 * half_slots, 128), bf16),
        ],
        1_000_000,
        (place, expert_ids, route_share[:, None], tokens, upstream),
    )
    token_block, grad_block = call(
        pack_kernel,
        1,
        [whole((half_slots, block))] * 2 + [whole((half_slots, 128))],
        [whole((rows, block + 128)), whole((rows, block))],
        [
            jax.ShapeDtypeStruct((rows, block + 128), bf16),
            jax.ShapeDtypeStruct((rows, block), bf16),
        ],
        [],
        1_000_000,
        (place, mine, swap(theirs), meta),
    )

    def to_experts(block_rows):
        width = block_rows.shape[1]
        return exchange(block_rows.reshape(ep_size, half_cap, width)).reshape(rows, width)

    token_full = to_experts(token_block)
    grad_rows = to_experts(grad_block)

    head = lax.all_gather(reward_head, TP, axis=0, tiled=True)
    head_own = jnp.sum(w_down.astype(f32) * head[None, :], axis=1)
    head_other = jnp.sum(wd_other.astype(f32) * head[None, :], axis=1)
    head_row = jnp.concatenate([head_own, head_other])[None, :]
    local_scores = jnp.sum(tokens.astype(f32) * reward_head[None, :], axis=1)
    local_rewards = jnp.sum(local_scores.reshape(seq_local, SEQ_LEN), axis=1)
    seq_total = pair_order.shape[0]
    offset = lax.axis_index(EP) * seq_local
    placed = lax.dynamic_update_slice(jnp.zeros((seq_total,), f32), local_rewards, (offset,))
    token_full, head_row, placed = lax.optimization_barrier((token_full, head_row, placed))

    token_pieces = gather_features(token_full[:, :block])
    grad_pieces = gather_features(grad_rows)

    slots_hid = (rows, 2 * hid)
    meta_spec = pl.BlockSpec((rows, 128), lambda k, y: (0, block // 128))
    work = rows * 2 * hid * 4 * block
    own_rows, ahead_rows, far_low, far_high, back_rows = token_pieces
    gate_weights = (w_gate, wg_other, w_up, wu_other)
    full, part = whole((rows, block)), whole((rows // 2, block))
    gate, up = call(
        near_kernel,
        3,
        [full] * 3 + [near_columns(hid, block)] * 4,
        [whole(slots_hid)] * 2,
        [jax.ShapeDtypeStruct(slots_hid, f32)] * 2,
        [pltpu.VMEM((rows, block), bf16)],
        3 * work,
        (place, own_rows, ahead_rows, back_rows, *gate_weights),
    )
    slope, silu, hidden, score = call(
        fwd_kernel,
        1,
        [part] * 2
        + [far_columns(hid, block)] * 4
        + [whole((1, 2 * hid)), meta_spec]
        + [whole(slots_hid)] * 2,
        [whole(slots_hid)] * 3 + [whole((ep_size, 128))],
        [jax.ShapeDtypeStruct(slots_hid, f32)] * 2
        + [jax.ShapeDtypeStruct(slots_hid, bf16), jax.ShapeDtypeStruct((ep_size, 128), f32)],
        [pltpu.VMEM(slots_hid, f32)] * 2 + [pltpu.VMEM((rows, block), bf16)],
        work,
        (place, far_low, far_high, *gate_weights, head_row, token_full, gate, up),
    )
    placed = (placed + score[:, :seq_local].reshape(seq_total)).reshape(2, 1, seq_total // 2)
    everyone = lax.axis_size(EP_TP)
    spread = jnp.broadcast_to(placed, (2, everyone, seq_total // 2))
    spread = lax.all_to_all(spread, EP_TP, split_axis=1, concat_axis=1, tiled=True)
    rewards = jnp.sum(spread, axis=1).reshape(seq_total) / math.sqrt(SEQ_LEN)

    half_shape = jax.ShapeDtypeStruct((rows // 2, block), bf16)
    full_shape = jax.ShapeDtypeStruct((rows, block), bf16)
    down_low, down_high = call(
        down_kernel,
        1,
        [whole(slots_hid)] + [far_columns(hid, block)] * 2,
        [part] * 2,
        [half_shape] * 2,
        [],
        work // 2,
        (place, hidden, w_down, wd_other),
    )
    down_own, down_ahead, down_back = call(
        side_kernel,
        3,
        [whole(slots_hid)] + [near_columns(hid, block)] * 2,
        [full] * 3,
        [full_shape] * 3,
        [pltpu.VMEM((rows, block), bf16)],
        3 * work // 2,
        (place, hidden, w_down, wd_other),
    )
    down_pieces = (down_own, down_ahead, down_low, down_high, down_back)
    partial = call(
        back_kernel,
        4,
        piece_specs(rows, block) + [columns(hid, block)] * 2,
        [whole(slots_hid)],
        [jax.ShapeDtypeStruct(slots_hid, f32)],
        [pltpu.VMEM((rows, block), bf16)],
        2 * work,
        (place, *grad_pieces, w_down, wd_other),
    )[0]
    down_sums = scatter_start(down_pieces)

    seq_iota = jnp.arange(seq_total, dtype=jnp.int32)
    chosen_hot = (pair_order[0::2][:, None] == seq_iota[None, :]).astype(f32)
    rejected_hot = (pair_order[1::2][:, None] == seq_iota[None, :]).astype(f32)
    margin = jnp.sum((chosen_hot - rejected_hot) * rewards[None, :], axis=1)
    pair_loss = jnp.mean(jax.nn.softplus(-margin))
    pair_weight = jax.nn.sigmoid(-margin)
    seq_coef = jnp.sum(pair_weight[:, None] * (rejected_hot - chosen_hot), axis=0)
    token_coef = jnp.repeat(lax.dynamic_slice_in_dim(seq_coef, offset, seq_local), SEQ_LEN)
    grad_out = (
        upstream.astype(f32)
        + loss_scale * token_coef[:, None] * reward_head[None, :] / math.sqrt(SEQ_LEN)
    ).astype(bf16)
    scaled = (seq_coef * (loss_scale / math.sqrt(SEQ_LEN))).reshape(ep_size, seq_local)

    gate_grad, up_grad, slot_coef, far_low, far_high = call(
        bwd_kernel,
        1,
        [far_columns(hid, block)] * 4
        + [whole((1, 2 * hid)), meta_spec, whole((ep_size, seq_local))]
        + [whole(slots_hid)] * 3,
        [whole(slots_hid)] * 2 + [whole((rows, 1))] + [part] * 2,
        [jax.ShapeDtypeStruct(slots_hid, bf16)] * 2
        + [jax.ShapeDtypeStruct((rows, 1), f32)]
        + [jax.ShapeDtypeStruct((rows // 2, block), bf16)] * 2,
        [],
        work,
        (place, *gate_weights, head_row, token_full, scaled, partial, slope, silu),
    )
    own_sums, ahead_sums, back_sums = call(
        rest_kernel,
        3,
        [near_columns(hid, block)] * 4 + [whole(slots_hid)] * 2,
        [full] * 3,
        [jax.ShapeDtypeStruct((rows, block), bf16)] * 3,
        [pltpu.VMEM((rows, block), bf16)],
        3 * work,
        (place, *gate_weights, gate_grad, up_grad),
    )
    input_sums = scatter_start((own_sums, ahead_sums, far_low, far_high, back_sums))

    own_grads, other_grads = call(
        grad_kernel,
        4,
        piece_specs(rows, block) * 2
        + [whole(slots_hid)] * 3
        + [whole((rows, 1)), columns(1, block)],
        [columns(3 * hid, block)] * 2,
        [jax.ShapeDtypeStruct((3 * hid, 4 * block), bf16)] * 2,
        [pltpu.VMEM((6, hid, rows), bf16), pltpu.VMEM((2, rows, block), bf16)],
        6 * work,
        (place, *token_pieces, *grad_pieces, hidden, gate_grad, up_grad, slot_coef, head[None, :]),
    )
    other_grads = swap(other_grads)
    grad_gate, grad_up, grad_down = (
        add(own_grads[i * hid : (i + 1) * hid], other_grads[i * hid : (i + 1) * hid])
        for i in range(3)
    )

    def come_back(pieces):
        summed = add(*pieces).reshape(ep_size, half_cap, block)
        arrived = exchange(summed).astype(f32)
        sums = jnp.sum(arrived.reshape(EXPERTS, replicas, half_cap, block), axis=1)
        sums = sums.astype(bf16).reshape(EXPERTS * half_cap, block)
        left, right = sums[:, :local_width], sums[:, local_width:]
        mine = jnp.where(core == 0, left, right)
        theirs = swap(jnp.where(core == 0, right, left))
        return jnp.concatenate(
            [jnp.where(core == 0, mine, theirs), jnp.where(core == 0, theirs, mine)], axis=0
        )

    mixed_sum = plain(mixing, come_back(down_sums).astype(f32))
    layer_out = (tokens.astype(f32) + mixed_sum).astype(bf16)
    returned = plain(picker, come_back(input_sums))
    grad_tokens = (grad_out.astype(f32) + returned).astype(bf16)
    return (layer_out, rewards, pair_loss, grad_tokens, grad_gate, grad_up, grad_down)


def solution(mesh):
    split = Mesh(mesh.devices.reshape(4, 8, 4, 2), EP_TP)
    in_specs = (
        P(EP, TP),
        P(EP, None),
        P(EP),
        P(EP_TP, None),
        P(EP_TP, None),
        P(EP_TP, None),
        P(TP),
        P(EP, TP),
        P(),
    )
    out_specs = (P(EP, TP), P(), P(), P(EP, TP), P(EP_TP, None), P(EP_TP, None), P(EP_TP, None))
    return jax.shard_map(layer, mesh=split, in_specs=in_specs, out_specs=out_specs, check_vma=False)
```

```python
import math

import jax
import jax.numpy as jnp
from jax import lax
from jax.experimental import pallas as pl
from jax.experimental.pallas import tpu as pltpu
from jax.sharding import Mesh
from jax.sharding import PartitionSpec as P


EXPERTS = 8
SEQ_LEN = 64
EP = ("ep_x", "ep_z")
TP = ("tp_y", "tp_c")
EP_TP = EP + TP


loss_scale = 256.0
VMEM_MIB = 60
bf16, f32 = jnp.bfloat16, jnp.float32


def route_kernel(at_ref, ids_ref, share_ref, tokens_ref, upstream_ref, *refs):
    mine_ref, theirs_ref, meta_ref, picker_ref, mixing_ref, both, meta = refs
    slots, count = picker_ref.shape
    local_width = tokens_ref.shape[1]
    half_cap = slots // (2 * EXPERTS)
    lane = lax.broadcasted_iota(jnp.int32, (count, count), 1)
    row = lax.broadcasted_iota(jnp.int32, (count, count), 0)
    earlier = (row < lane).astype(f32).astype(bf16)
    expert = lax.broadcasted_iota(jnp.int32, (2 * EXPERTS, count), 0)
    hot = [(expert == ids_ref[pl.ds(i, 1)]).astype(f32) for i in (0, 1)]
    before = [plain(h.astype(bf16), earlier) for h in hot]
    before[1] = before[1] + jnp.sum(hot[0], axis=1, keepdims=True)
    slot_iota = lax.broadcasted_iota(jnp.int32, (slots, count), 0)
    share = share_ref[...]
    picker = jnp.zeros((slots, count), f32)
    shares = jnp.zeros((slots, count), f32)
    for i, weight in ((0, share), (1, 1.0 - share)):
        rank = jnp.sum(before[i] * hot[i], axis=0, keepdims=True).astype(jnp.int32)
        late = (rank >= half_cap).astype(jnp.int32)
        slot = late * (slots // 2 - half_cap) + ids_ref[pl.ds(i, 1)] * half_cap + rank
        slot = jnp.where(rank < 2 * half_cap, slot, -1)
        match = (slot_iota == slot).astype(f32)
        picker = picker + match
        shares = shares + match * weight
    by_slot = picker.astype(bf16)
    picker_ref[...] = by_slot
    mixing_ref[...] = shares
    slot_share = jnp.sum(shares, axis=1, keepdims=True)
    both[:, pl.ds(0, local_width)] = plain(by_slot, tokens_ref[...]).astype(bf16)
    both[:, pl.ds(local_width, local_width)] = (
        plain(by_slot, upstream_ref[...]) * slot_share
    ).astype(bf16)
    lane = lax.broadcasted_iota(jnp.int32, (slots, count), 1)
    table = jnp.zeros((slots, count), f32)
    for seq in range(count // SEQ_LEN):
        part = jnp.where(lane // SEQ_LEN == seq, shares, 0.0)
        part = jnp.sum(part, axis=1, keepdims=True)
        high = part.astype(bf16).astype(f32)
        table = jnp.where(lane == 2 * seq, high, table)
        table = jnp.where(lane == 2 * seq + 1, part - high, table)
    meta[...] = table.astype(bf16)
    half = slots // 2
    core = at_ref[1]
    own = pl.ds(pl.multiple_of(core * half, half), half)
    other = pl.ds(pl.multiple_of((1 - core) * half, half), half)
    mine_ref[...] = both[own]
    theirs_ref[...] = both[other]
    meta_ref[...] = meta[own]


def pack_kernel(at_ref, mine_ref, got_ref, *refs):
    out_ref = refs[-1]
    start = 0 if len(refs) == 1 else mine_ref.shape[1] // 2
    local_width = mine_ref.shape[1] // 2
    half_cap = mine_ref.shape[0] // EXPERTS
    replicas = out_ref.shape[0] // mine_ref.shape[0]
    columns = pl.ds(start, local_width)
    for core in (0, 1):
        low, high = (mine_ref, got_ref) if core == 0 else (got_ref, mine_ref)

        @pl.when(at_ref[1] == core)
        def _(low=low, high=high):
            for i in range(EXPERTS * replicas):
                src = pl.ds(i // replicas * half_cap, half_cap)
                dst = pl.ds(i * half_cap, half_cap)
                out_ref[dst, pl.ds(0, local_width)] = low[src, columns]
                out_ref[dst, pl.ds(local_width, local_width)] = high[src, columns]
                for meta_ref in refs[:-1]:
                    out_ref[dst, pl.ds(2 * local_width, 128)] = meta_ref[src]


def rot(value, shift):
    return lax.ppermute(value, "tp_y", [(i, (i + shift) % 4) for i in range(4)])


def swap(value):
    return lax.ppermute(value, "tp_c", [(0, 1), (1, 0)])


def exchange(blocks):
    arrived = lax.all_to_all(
        blocks.transpose(1, 0, 2), EP, split_axis=1, concat_axis=1, tiled=True
    )
    return arrived.transpose(1, 0, 2)


def gather_features(rows):
    half = rows.shape[0] // 2
    back, ahead = rot(rows, 1), rot(rows, -1)
    far_low, far_high = rot(back[:half], 1), rot(ahead[half:], -1)
    return (rows, ahead, far_low, far_high, back)


def add(*terms):
    return sum((t.astype(f32) for t in terms[1:]), terms[0].astype(f32)).astype(bf16)


def scatter_start(pieces):
    own, ahead, far_low, far_high, back = pieces
    half = far_low.shape[0]
    via_low, via_high = rot(far_low, 1), rot(far_high, -1)
    onward = add(ahead, jnp.pad(via_low, ((0, half), (0, 0))))
    backward = add(back, jnp.pad(via_high, ((half, 0), (0, 0))))
    return own, rot(onward, 1), rot(backward, -1)


def piece_halves(refs):
    own, ahead, far_low, far_high, back = refs
    half = far_low.shape[0]
    low, high = pl.ds(0, half), pl.ds(half, half)
    return (
        (own.at[low], own.at[high]),
        (ahead.at[low], ahead.at[high]),
        (far_low, far_high),
        (back.at[low], back.at[high]),
    )


def load_piece(step, refs, rows):
    half = rows.shape[0] // 2
    for k, (low, high) in enumerate(piece_halves(refs)):

        @pl.when(step == k)
        def _(low=low, high=high):
            rows[pl.ds(0, half)] = low[...]
            rows[pl.ds(half, half)] = high[...]


def cross(a, b):
    return lax.dot_general(a, b, (((1,), (1,)), ((), ())), preferred_element_type=f32)


def across(a, b):
    return lax.dot_general(a, b, (((0,), (0,)), ((), ())), preferred_element_type=f32)


def plain(a, b):
    return lax.dot_general(a, b, (((1,), (0,)), ((), ())), preferred_element_type=f32)


def near_kernel(y_ref, *refs):
    x_refs = refs[:3]
    weights, accs, rows = refs[3:7], refs[7:9], refs[9]
    width = weights[0].shape[0]
    step = pl.program_id(0)

    @pl.when(step == 0)
    def _():
        for acc in accs:
            acc[...] = jnp.zeros_like(acc)

    for k, ref in enumerate(x_refs):

        @pl.when(step == k)
        def _(ref=ref):
            rows[...] = ref[...]

    chunk = rows.shape[0] // 2

    @pl.loop(0, 2)
    def _(i):
        at = pl.ds(pl.multiple_of(i * chunk, chunk), chunk)
        for j, weight in enumerate(weights):
            accs[j // 2][at, pl.ds(j % 2 * width, width)] += cross(rows[at], weight[...])


def fwd_kernel(y_ref, *refs):
    far_refs = refs[:2]
    wg0, wg1, wu0, wu1, rh_ref, meta_ref, gate_ref, up_ref = refs[2:10]
    slope_ref, silu_ref, hidden_ref, score_ref = refs[10:14]
    gate_acc, up_acc, rows = refs[14:]
    half, width = rows.shape[0] // 2, wg0.shape[0]
    left, right = pl.ds(0, width), pl.ds(width, width)
    rows[pl.ds(0, half)] = far_refs[0][...]
    rows[pl.ds(half, half)] = far_refs[1][...]
    gate_acc[:, left] = gate_ref[:, left] + cross(rows[...], wg0[...])
    gate_acc[:, right] = gate_ref[:, right] + cross(rows[...], wg1[...])
    up_acc[:, left] = up_ref[:, left] + cross(rows[...], wu0[...])
    up_acc[:, right] = up_ref[:, right] + cross(rows[...], wu1[...])
    finish_forward(
        rh_ref, meta_ref, slope_ref, silu_ref, hidden_ref, score_ref, gate_acc, up_acc
    )


def finish_forward(
    rh_ref, meta_ref, slope_ref, silu_ref, hidden_ref, score_ref, gate_acc, up_acc
):
    chunk = gate_acc.shape[0] // 8

    @pl.loop(0, 8)
    def _(i):
        at = pl.ds(pl.multiple_of(i * chunk, chunk), chunk)
        gate, up = gate_acc[at], up_acc[at]
        sig = jax.nn.sigmoid(gate)
        silu = gate * sig
        hidden = (silu * up).astype(bf16)
        silu_ref[at] = silu
        slope_ref[at] = up * (sig * (1.0 + gate * (1.0 - sig)))
        hidden_ref[at] = hidden
        score = jnp.sum(hidden.astype(f32) * rh_ref[...], axis=1, keepdims=True)
        gate_acc[at, pl.ds(0, 128)] = score * meta_ref[at].astype(f32)

    scores = gate_acc[:, pl.ds(0, 128)].reshape(score_ref.shape[0], -1, 128)
    scores = jnp.sum(scores, axis=1)
    lane = lax.broadcasted_iota(jnp.int32, scores.shape, 1)
    first = jnp.sum(jnp.where(lane < 2, scores, 0.0), axis=1, keepdims=True)
    second = jnp.sum(jnp.where(lane < 2, 0.0, scores), axis=1, keepdims=True)
    score_ref[...] = jnp.where(lane == 0, first, second)


def down_kernel(y_ref, hidden_ref, wd0, wd1, low_ref, high_ref):
    width, half = wd0.shape[0], low_ref.shape[0]
    left, right = pl.ds(0, width), pl.ds(width, width)
    for i, ref in enumerate((low_ref, high_ref)):
        at = pl.ds(i * half, half)
        ref[...] = (
            plain(hidden_ref[at, left], wd0[...]) + plain(hidden_ref[at, right], wd1[...])
        ).astype(bf16)


def side_kernel(y_ref, hidden_ref, wd0, wd1, *refs):
    out_refs, rows = refs[:3], refs[3]
    width = wd0.shape[0]
    left, right = pl.ds(0, width), pl.ds(width, width)
    chunk = rows.shape[0] // 2

    @pl.loop(0, 2)
    def _(i):
        at = pl.ds(pl.multiple_of(i * chunk, chunk), chunk)
        rows[at] = (
            plain(hidden_ref[at, left], wd0[...]) + plain(hidden_ref[at, right], wd1[...])
        ).astype(bf16)

    for k, ref in enumerate(out_refs):

        @pl.when(pl.program_id(0) == k)
        def _(ref=ref):
            ref[...] = rows[...]


def back_kernel(y_ref, *refs):
    u_refs, (wd0, wd1, out_ref, rows) = refs[:5], refs[5:]
    width = wd0.shape[0]
    left, right = pl.ds(0, width), pl.ds(width, width)
    step = pl.program_id(0)

    @pl.when(step == 0)
    def _():
        out_ref[...] = jnp.zeros_like(out_ref)

    load_piece(step, u_refs, rows)
    out_ref[:, left] += cross(rows[...], wd0[...])
    out_ref[:, right] += cross(rows[...], wd1[...])


def bwd_kernel(y_ref, *refs):
    wg0, wg1, wu0, wu1, rh_ref, meta_ref, seq_ref, partial_ref, slope_ref, silu_ref = refs[:10]
    gate_grad_ref, up_grad_ref, coef_ref, low_ref, high_ref = refs[10:15]
    width, half = wg0.shape[0], low_ref.shape[0]
    left, right = pl.ds(0, width), pl.ds(width, width)
    count = partial_ref.shape[0]
    blocks = seq_ref.shape[0]
    lane = lax.broadcasted_iota(jnp.int32, (blocks, 128), 1)
    first = jnp.broadcast_to(seq_ref[:, pl.ds(0, 1)], lane.shape)
    second = jnp.broadcast_to(seq_ref[:, pl.ds(1, 1)], lane.shape)
    by_lane = jnp.where(lane < 2, first, jnp.where(lane < 4, second, 0.0))
    shares = meta_ref[...].astype(f32).reshape(blocks, count // blocks, 128)
    terms = (shares * by_lane[:, None, :]).reshape(count, 128)
    coef_ref[...] = jnp.sum(terms, axis=1, keepdims=True)
    chunk = count // 8

    @pl.loop(0, 8)
    def _(i):
        at = pl.ds(pl.multiple_of(i * chunk, chunk), chunk)
        hidden_grad = partial_ref[at] + coef_ref[at] * rh_ref[...]
        gate_grad_ref[at] = (hidden_grad * slope_ref[at]).astype(bf16)
        up_grad_ref[at] = (hidden_grad * silu_ref[at]).astype(bf16)

    for i, ref in enumerate((low_ref, high_ref)):
        at = pl.ds(i * half, half)
        ref[...] = (
            plain(gate_grad_ref[at, left], wg0[...])
            + plain(gate_grad_ref[at, right], wg1[...])
            + plain(up_grad_ref[at, left], wu0[...])
            + plain(up_grad_ref[at, right], wu1[...])
        ).astype(bf16)


def rest_kernel(y_ref, *refs):
    wg0, wg1, wu0, wu1, gate_grad_ref, up_grad_ref = refs[:6]
    out_refs, rows = refs[6:9], refs[9]
    width = wg0.shape[0]
    left, right = pl.ds(0, width), pl.ds(width, width)
    chunk = rows.shape[0] // 2

    @pl.loop(0, 2)
    def _(i):
        at = pl.ds(pl.multiple_of(i * chunk, chunk), chunk)
        rows[at] = (
            plain(gate_grad_ref[at, left], wg0[...])
            + plain(gate_grad_ref[at, right], wg1[...])
            + plain(up_grad_ref[at, left], wu0[...])
            + plain(up_grad_ref[at, right], wu1[...])
        ).astype(bf16)

    for k, ref in enumerate(out_refs):

        @pl.when(pl.program_id(0) == k)
        def _(ref=ref):
            ref[...] = rows[...]


def grad_kernel(y_ref, *refs):
    x_refs, u_refs = refs[:5], refs[5:10]
    hidden_ref, gate_grad_ref, up_grad_ref, coef_ref, rh_ref = refs[10:15]
    own_ref, other_ref, left, rows = refs[15:]
    width = left.shape[1]
    step = pl.program_id(0)

    @pl.when(step == 0)
    def _():
        for i, ref in enumerate((gate_grad_ref, up_grad_ref, hidden_ref)):
            turned = ref[...].T
            left[2 * i] = turned[:width]
            left[2 * i + 1] = turned[width:]

    load_piece(step, x_refs, rows.at[0])
    load_piece(step, u_refs, rows.at[1])
    rows[1] = (rows[1].astype(f32) + coef_ref[...] * rh_ref[...]).astype(bf16)

    @pl.loop(0, 3)
    def _(i):
        at = pl.ds(pl.multiple_of(i * width, width), width)
        own_ref[at] = plain(left[2 * i], rows[i // 2]).astype(bf16)
        other_ref[at] = plain(left[2 * i + 1], rows[i // 2]).astype(bf16)


def whole(shape):
    return pl.BlockSpec(shape, lambda k, y: (0,) * len(shape))


def columns(width, block):
    return pl.BlockSpec((width, block), lambda k, y: (0, (y[0] + k) % 4))


def near_columns(width, block):
    return pl.BlockSpec((width, block), lambda k, y: (0, (y[0] + k + k // 2) % 4))


def far_columns(width, block):
    return pl.BlockSpec((width, block), lambda k, y: (0, (y[0] + 2) % 4))


def piece_specs(rows, block):
    full, part = whole((rows, block)), whole((rows // 2, block))
    return [full, full, part, part, full]


def call(kernel, steps, in_specs, out_specs, out_shape, scratch, flops, args):
    return pl.pallas_call(
        kernel,
        grid_spec=pltpu.PrefetchScalarGridSpec(
            num_scalar_prefetch=1,
            grid=(steps,),
            in_specs=in_specs,
            out_specs=out_specs,
            scratch_shapes=scratch,
        ),
        out_shape=out_shape,
        compiler_params=pltpu.CompilerParams(
            dimension_semantics=("arbitrary",), vmem_limit_bytes=VMEM_MIB * 1024 * 1024
        ),
        cost_estimate=pl.CostEstimate(flops=flops, bytes_accessed=20_000_000, transcendentals=0),
    )(*args)


def layer(
    tokens, expert_ids, route_share, w_gate, w_up, w_down, reward_head, upstream, pair_order
):
    tok_count, local_width = tokens.shape
    capacity = tok_count * expert_ids.shape[1] // EXPERTS
    ep_size = lax.axis_size(EP)
    replicas = ep_size // EXPERTS
    half_cap = capacity // 2
    block = 2 * local_width
    rows = ep_size * half_cap
    hid = w_gate.shape[0]
    core = lax.axis_index("tp_c")
    place = jnp.stack([lax.axis_index("tp_y"), core]).astype(jnp.int32)

    wg_other, wu_other, wd_other = swap(w_gate), swap(w_up), swap(w_down)

    seq_local = tok_count // SEQ_LEN
    half_slots = EXPERTS * half_cap
    half_rows = jax.ShapeDtypeStruct((half_slots, block), bf16)
    mine, theirs, meta, picker, mixing = call(
        route_kernel,
        1,
        [whole((2, tok_count)), whole((1, tok_count))] + [whole((tok_count, local_width))] * 2,
        [whole((half_slots, block))] * 2
        + [whole((half_slots, 128))]
        + [whole((2 * half_slots, tok_count))] * 2,
        [
            half_rows,
            half_rows,
            jax.ShapeDtypeStruct((half_slots, 128), bf16),
            jax.ShapeDtypeStruct((2 * half_slots, tok_count), bf16),
            jax.ShapeDtypeStruct((2 * half_slots, tok_count), f32),
        ],
        [
            pltpu.VMEM((2 * half_slots, block), bf16),
            pltpu.VMEM((2 * half_slots, 128), bf16),
        ],
        1_000_000,
        (place, expert_ids.T, route_share[None, :], tokens, upstream),
    )
    theirs = swap(theirs)
    half_spec = whole((half_slots, block))
    token_block = call(
        pack_kernel,
        1,
        [half_spec] * 2,
        whole((rows, block)),
        jax.ShapeDtypeStruct((rows, block), bf16),
        [],
        1_000_000,
        (place, mine, theirs),
    )
    grad_block = call(
        pack_kernel,
        1,
        [half_spec] * 2 + [whole((half_slots, 128))],
        whole((rows, block + 128)),
        jax.ShapeDtypeStruct((rows, block + 128), bf16),
        [],
        1_000_000,
        (place, mine, theirs, meta),
    )

    def to_experts(block_rows):
        width = block_rows.shape[1]
        return exchange(block_rows.reshape(ep_size, half_cap, width)).reshape(rows, width)

    token_rows = to_experts(token_block)
    grad_full = to_experts(grad_block)

    head = lax.all_gather(reward_head, TP, axis=0, tiled=True)
    head_own = jnp.sum(w_down.astype(f32) * head[None, :], axis=1)
    head_other = jnp.sum(wd_other.astype(f32) * head[None, :], axis=1)
    head_row = jnp.concatenate([head_own, head_other])[None, :]
    local_scores = jnp.sum(tokens.astype(f32) * reward_head[None, :], axis=1)
    local_rewards = jnp.sum(local_scores.reshape(seq_local, SEQ_LEN), axis=1)
    seq_total = pair_order.shape[0]
    offset = lax.axis_index(EP) * seq_local
    placed = lax.dynamic_update_slice(jnp.zeros((seq_total,), f32), local_rewards, (offset,))
    token_rows, head_row, placed = lax.optimization_barrier((token_rows, head_row, placed))

    token_pieces = gather_features(token_rows)
    grad_pieces = gather_features(grad_full[:, :block])

    slots_hid = (rows, 2 * hid)
    meta_spec = pl.BlockSpec((rows, 128), lambda k, y: (0, block // 128))
    work = rows * 2 * hid * 4 * block
    own_rows, ahead_rows, far_low, far_high, back_rows = token_pieces
    gate_weights = (w_gate, wg_other, w_up, wu_other)
    full, part = whole((rows, block)), whole((rows // 2, block))
    gate, up = call(
        near_kernel,
        3,
        [full] * 3 + [near_columns(hid, block)] * 4,
        [whole(slots_hid)] * 2,
        [jax.ShapeDtypeStruct(slots_hid, f32)] * 2,
        [pltpu.VMEM((rows, block), bf16)],
        3 * work,
        (place, own_rows, ahead_rows, back_rows, *gate_weights),
    )
    slope, silu, hidden, score = call(
        fwd_kernel,
        1,
        [part] * 2
        + [far_columns(hid, block)] * 4
        + [whole((1, 2 * hid)), meta_spec]
        + [whole(slots_hid)] * 2,
        [whole(slots_hid)] * 3 + [whole((ep_size, 128))],
        [jax.ShapeDtypeStruct(slots_hid, f32)] * 2
        + [jax.ShapeDtypeStruct(slots_hid, bf16), jax.ShapeDtypeStruct((ep_size, 128), f32)],
        [pltpu.VMEM(slots_hid, f32)] * 2 + [pltpu.VMEM((rows, block), bf16)],
        work,
        (place, far_low, far_high, *gate_weights, head_row, grad_full, gate, up),
    )
    placed = (placed + score[:, :seq_local].reshape(seq_total)).reshape(2, 1, seq_total // 2)
    everyone = lax.axis_size(EP_TP)
    spread = jnp.broadcast_to(placed, (2, everyone, seq_total // 2))
    spread = lax.all_to_all(spread, EP_TP, split_axis=1, concat_axis=1, tiled=True)
    rewards = jnp.sum(spread, axis=1).reshape(seq_total) / math.sqrt(SEQ_LEN)

    half_shape = jax.ShapeDtypeStruct((rows // 2, block), bf16)
    full_shape = jax.ShapeDtypeStruct((rows, block), bf16)
    down_low, down_high = call(
        down_kernel,
        1,
        [whole(slots_hid)] + [far_columns(hid, block)] * 2,
        [part] * 2,
        [half_shape] * 2,
        [],
        work // 2,
        (place, hidden, w_down, wd_other),
    )
    down_own, down_ahead, down_back = call(
        side_kernel,
        3,
        [whole(slots_hid)] + [near_columns(hid, block)] * 2,
        [full] * 3,
        [full_shape] * 3,
        [pltpu.VMEM((rows, block), bf16)],
        3 * work // 2,
        (place, hidden, w_down, wd_other),
    )
    down_pieces = (down_own, down_ahead, down_low, down_high, down_back)
    partial = call(
        back_kernel,
        4,
        piece_specs(rows, block) + [columns(hid, block)] * 2,
        [whole(slots_hid)],
        [jax.ShapeDtypeStruct(slots_hid, f32)],
        [pltpu.VMEM((rows, block), bf16)],
        2 * work,
        (place, *grad_pieces, w_down, wd_other),
    )[0]
    down_sums = scatter_start(down_pieces)

    seq_iota = jnp.arange(seq_total, dtype=jnp.int32)
    chosen_hot = (pair_order[0::2][:, None] == seq_iota[None, :]).astype(f32)
    rejected_hot = (pair_order[1::2][:, None] == seq_iota[None, :]).astype(f32)
    margin = jnp.sum((chosen_hot - rejected_hot) * rewards[None, :], axis=1)
    pair_loss = jnp.mean(jax.nn.softplus(-margin))
    pair_weight = jax.nn.sigmoid(-margin)
    seq_coef = jnp.sum(pair_weight[:, None] * (rejected_hot - chosen_hot), axis=0)
    token_coef = jnp.repeat(lax.dynamic_slice_in_dim(seq_coef, offset, seq_local), SEQ_LEN)
    grad_out = (
        upstream.astype(f32)
        + loss_scale * token_coef[:, None] * reward_head[None, :] / math.sqrt(SEQ_LEN)
    ).astype(bf16)
    scaled = (seq_coef * (loss_scale / math.sqrt(SEQ_LEN))).reshape(ep_size, seq_local)

    gate_grad, up_grad, slot_coef, far_low, far_high = call(
        bwd_kernel,
        1,
        [far_columns(hid, block)] * 4
        + [whole((1, 2 * hid)), meta_spec, whole((ep_size, seq_local))]
        + [whole(slots_hid)] * 3,
        [whole(slots_hid)] * 2 + [whole((rows, 1))] + [part] * 2,
        [jax.ShapeDtypeStruct(slots_hid, bf16)] * 2
        + [jax.ShapeDtypeStruct((rows, 1), f32)]
        + [jax.ShapeDtypeStruct((rows // 2, block), bf16)] * 2,
        [],
        work,
        (place, *gate_weights, head_row, grad_full, scaled, partial, slope, silu),
    )
    own_sums, ahead_sums, back_sums = call(
        rest_kernel,
        3,
        [near_columns(hid, block)] * 4 + [whole(slots_hid)] * 2,
        [full] * 3,
        [jax.ShapeDtypeStruct((rows, block), bf16)] * 3,
        [pltpu.VMEM((rows, block), bf16)],
        3 * work,
        (place, *gate_weights, gate_grad, up_grad),
    )
    input_sums = scatter_start((own_sums, ahead_sums, far_low, far_high, back_sums))

    own_grads, other_grads = call(
        grad_kernel,
        4,
        piece_specs(rows, block) * 2
        + [whole(slots_hid)] * 3
        + [whole((rows, 1)), columns(1, block)],
        [columns(3 * hid, block)] * 2,
        [jax.ShapeDtypeStruct((3 * hid, 4 * block), bf16)] * 2,
        [pltpu.VMEM((6, hid, rows), bf16), pltpu.VMEM((2, rows, block), bf16)],
        6 * work,
        (place, *token_pieces, *grad_pieces, hidden, gate_grad, up_grad, slot_coef, head[None, :]),
    )
    other_grads = swap(other_grads)
    grad_gate, grad_up, grad_down = (
        add(own_grads[i * hid : (i + 1) * hid], other_grads[i * hid : (i + 1) * hid])
        for i in range(3)
    )

    def come_back(pieces):
        summed = add(*pieces).reshape(ep_size, half_cap, block)
        arrived = exchange(summed).astype(f32)
        sums = jnp.sum(arrived.reshape(EXPERTS, replicas, half_cap, block), axis=1)
        sums = sums.astype(bf16).reshape(EXPERTS * half_cap, block)
        left, right = sums[:, :local_width], sums[:, local_width:]
        mine = jnp.where(core == 0, left, right)
        theirs = swap(jnp.where(core == 0, right, left))
        return jnp.concatenate(
            [jnp.where(core == 0, mine, theirs), jnp.where(core == 0, theirs, mine)], axis=0
        )

    mixed_sum = across(mixing, come_back(down_sums).astype(f32))
    layer_out = (tokens.astype(f32) + mixed_sum).astype(bf16)
    returned = across(picker, come_back(input_sums))
    grad_tokens = (grad_out.astype(f32) + returned).astype(bf16)
    return (layer_out, rewards, pair_loss, grad_tokens, grad_gate, grad_up, grad_down)


def solution(mesh):
    split = Mesh(mesh.devices.reshape(4, 8, 4, 2), EP_TP)
    in_specs = (
        P(EP, TP),
        P(EP, None),
        P(EP),
        P(EP_TP, None),
        P(EP_TP, None),
        P(EP_TP, None),
        P(TP),
        P(EP, TP),
        P(),
    )
    out_specs = (P(EP, TP), P(), P(), P(EP, TP), P(EP_TP, None), P(EP_TP, None), P(EP_TP, None))
    return jax.shard_map(layer, mesh=split, in_specs=in_specs, out_specs=out_specs, check_vma=False)
```

```python
import math

import jax
import jax.numpy as jnp
from jax import lax
from jax.experimental import pallas as pl
from jax.experimental.pallas import tpu as pltpu
from jax.sharding import Mesh
from jax.sharding import PartitionSpec as P


EXPERTS = 8
SEQ_LEN = 64
EP = ("ep_x", "ep_z")
TP = ("tp_y", "tp_c")
EP_TP = EP + TP


loss_scale = 256.0
VMEM_MIB = 60
bf16, f32 = jnp.bfloat16, jnp.float32


def route_kernel(at_ref, ids_ref, share_ref, tokens_ref, upstream_ref, *refs):
    mine_ref, theirs_ref, meta_ref, picker_ref, mixing_ref, both, meta = refs
    slots, count = picker_ref.shape
    local_width = tokens_ref.shape[1]
    half_cap = slots // (2 * EXPERTS)
    lane = lax.broadcasted_iota(jnp.int32, (count, count), 1)
    row = lax.broadcasted_iota(jnp.int32, (count, count), 0)
    earlier = (row < lane).astype(f32).astype(bf16)
    expert = lax.broadcasted_iota(jnp.int32, (2 * EXPERTS, count), 0)
    hot = [(expert == ids_ref[pl.ds(i, 1)]).astype(f32) for i in (0, 1)]
    before = [plain(h.astype(bf16), earlier) for h in hot]
    before[1] = before[1] + jnp.sum(hot[0], axis=1, keepdims=True)
    slot_iota = lax.broadcasted_iota(jnp.int32, (slots, count), 0)
    share = share_ref[...]
    picker = jnp.zeros((slots, count), f32)
    shares = jnp.zeros((slots, count), f32)
    for i, weight in ((0, share), (1, 1.0 - share)):
        rank = jnp.sum(before[i] * hot[i], axis=0, keepdims=True).astype(jnp.int32)
        late = (rank >= half_cap).astype(jnp.int32)
        slot = late * (slots // 2 - half_cap) + ids_ref[pl.ds(i, 1)] * half_cap + rank
        slot = jnp.where(rank < 2 * half_cap, slot, -1)
        match = (slot_iota == slot).astype(f32)
        picker = picker + match
        shares = shares + match * weight
    by_slot = picker.astype(bf16)
    picker_ref[...] = by_slot
    mixing_ref[...] = shares
    slot_share = jnp.sum(shares, axis=1, keepdims=True)
    both[:, pl.ds(0, local_width)] = plain(by_slot, tokens_ref[...]).astype(bf16)
    both[:, pl.ds(local_width, local_width)] = (
        plain(by_slot, upstream_ref[...]) * slot_share
    ).astype(bf16)
    lane = lax.broadcasted_iota(jnp.int32, (slots, count), 1)
    table = jnp.zeros((slots, count), f32)
    for seq in range(count // SEQ_LEN):
        part = jnp.where(lane // SEQ_LEN == seq, shares, 0.0)
        part = jnp.sum(part, axis=1, keepdims=True)
        high = part.astype(bf16).astype(f32)
        table = jnp.where(lane == 2 * seq, high, table)
        table = jnp.where(lane == 2 * seq + 1, part - high, table)
    meta[...] = table.astype(bf16)
    half = slots // 2
    core = at_ref[1]
    own = pl.ds(pl.multiple_of(core * half, half), half)
    other = pl.ds(pl.multiple_of((1 - core) * half, half), half)
    mine_ref[...] = both[own]
    theirs_ref[...] = both[other]
    meta_ref[...] = meta[own]


def pack_kernel(at_ref, mine_ref, got_ref, *refs):
    out_ref = refs[-1]
    start = 0 if len(refs) == 1 else mine_ref.shape[1] // 2
    local_width = mine_ref.shape[1] // 2
    half_cap = mine_ref.shape[0] // EXPERTS
    replicas = out_ref.shape[0] // mine_ref.shape[0]
    columns = pl.ds(start, local_width)
    for core in (0, 1):
        low, high = (mine_ref, got_ref) if core == 0 else (got_ref, mine_ref)

        @pl.when(at_ref[1] == core)
        def _(low=low, high=high):
            for i in range(EXPERTS * replicas):
                src = pl.ds(i // replicas * half_cap, half_cap)
                dst = pl.ds(i * half_cap, half_cap)
                out_ref[dst, pl.ds(0, local_width)] = low[src, columns]
                out_ref[dst, pl.ds(local_width, local_width)] = high[src, columns]
                for meta_ref in refs[:-1]:
                    out_ref[dst, pl.ds(2 * local_width, 128)] = meta_ref[src]


def rot(value, shift):
    return lax.ppermute(value, "tp_y", [(i, (i + shift) % 4) for i in range(4)])


def swap(value):
    return lax.ppermute(value, "tp_c", [(0, 1), (1, 0)])


def exchange(blocks):
    arrived = lax.all_to_all(
        blocks.transpose(1, 0, 2), EP, split_axis=1, concat_axis=1, tiled=True
    )
    return arrived.transpose(1, 0, 2)


def gather_features(rows):
    half = rows.shape[0] // 2
    back, ahead = rot(rows, 1), rot(rows, -1)
    far_low, far_high = rot(back[:half], 1), rot(ahead[half:], -1)
    return (rows, ahead, far_low, far_high, back)


def add(*terms):
    return sum((t.astype(f32) for t in terms[1:]), terms[0].astype(f32)).astype(bf16)


def scatter_start(pieces):
    own, ahead, far_low, far_high, back = pieces
    half = far_low.shape[0]
    via_low, via_high = rot(far_low, 1), rot(far_high, -1)
    onward = add(ahead, jnp.pad(via_low, ((0, half), (0, 0))))
    backward = add(back, jnp.pad(via_high, ((half, 0), (0, 0))))
    return own, rot(onward, 1), rot(backward, -1)


def piece_halves(refs):
    own, ahead, far_low, far_high, back = refs
    half = far_low.shape[0]
    low, high = pl.ds(0, half), pl.ds(half, half)
    return (
        (own.at[low], own.at[high]),
        (ahead.at[low], ahead.at[high]),
        (far_low, far_high),
        (back.at[low], back.at[high]),
    )


def load_piece(step, refs, rows):
    half = rows.shape[0] // 2
    for k, (low, high) in enumerate(piece_halves(refs)):

        @pl.when(step == k)
        def _(low=low, high=high):
            rows[pl.ds(0, half)] = low[...]
            rows[pl.ds(half, half)] = high[...]


def cross(a, b):
    return lax.dot_general(a, b, (((1,), (1,)), ((), ())), preferred_element_type=f32)


def across(a, b):
    return lax.dot_general(a, b, (((0,), (0,)), ((), ())), preferred_element_type=f32)


def plain(a, b):
    return lax.dot_general(a, b, (((1,), (0,)), ((), ())), preferred_element_type=f32)


def near_kernel(y_ref, *refs):
    x_refs = refs[:3]
    weights, accs, rows = refs[3:7], refs[7:9], refs[9]
    width = weights[0].shape[0]
    step = pl.program_id(0)

    @pl.when(step == 0)
    def _():
        for acc in accs:
            acc[...] = jnp.zeros_like(acc)

    for k, ref in enumerate(x_refs):

        @pl.when(step == k)
        def _(ref=ref):
            rows[...] = ref[...]

    chunk = rows.shape[0] // 2

    @pl.loop(0, 2)
    def _(i):
        at = pl.ds(pl.multiple_of(i * chunk, chunk), chunk)
        for j, weight in enumerate(weights):
            accs[j // 2][at, pl.ds(j % 2 * width, width)] += cross(rows[at], weight[...])


def fwd_kernel(y_ref, *refs):
    far_refs = refs[:2]
    wg0, wg1, wu0, wu1, rh_ref, meta_ref, gate_ref, up_ref = refs[2:10]
    slope_ref, silu_ref, hidden_ref, score_ref = refs[10:14]
    gate_acc, up_acc, rows = refs[14:]
    half, width = rows.shape[0] // 2, wg0.shape[0]
    left, right = pl.ds(0, width), pl.ds(width, width)
    rows[pl.ds(0, half)] = far_refs[0][...]
    rows[pl.ds(half, half)] = far_refs[1][...]
    gate_acc[:, left] = gate_ref[:, left] + cross(rows[...], wg0[...])
    gate_acc[:, right] = gate_ref[:, right] + cross(rows[...], wg1[...])
    up_acc[:, left] = up_ref[:, left] + cross(rows[...], wu0[...])
    up_acc[:, right] = up_ref[:, right] + cross(rows[...], wu1[...])
    finish_forward(
        rh_ref, meta_ref, slope_ref, silu_ref, hidden_ref, score_ref, gate_acc, up_acc
    )


def finish_forward(
    rh_ref, meta_ref, slope_ref, silu_ref, hidden_ref, score_ref, gate_acc, up_acc
):
    chunk = gate_acc.shape[0] // 8

    @pl.loop(0, 8)
    def _(i):
        at = pl.ds(pl.multiple_of(i * chunk, chunk), chunk)
        gate, up = gate_acc[at], up_acc[at]
        sig = jax.nn.sigmoid(gate)
        silu = gate * sig
        hidden = (silu * up).astype(bf16)
        silu_ref[at] = silu
        slope_ref[at] = up * (sig * (1.0 + gate * (1.0 - sig)))
        hidden_ref[at] = hidden
        score = jnp.sum(hidden.astype(f32) * rh_ref[...], axis=1, keepdims=True)
        gate_acc[at, pl.ds(0, 128)] = score * meta_ref[at].astype(f32)

    scores = gate_acc[:, pl.ds(0, 128)].reshape(score_ref.shape[0], -1, 128)
    scores = jnp.sum(scores, axis=1)
    lane = lax.broadcasted_iota(jnp.int32, scores.shape, 1)
    first = jnp.sum(jnp.where(lane < 2, scores, 0.0), axis=1, keepdims=True)
    second = jnp.sum(jnp.where(lane < 2, 0.0, scores), axis=1, keepdims=True)
    score_ref[...] = jnp.where(lane == 0, first, second)


def down_kernel(y_ref, hidden_ref, wd0, wd1, low_ref, high_ref):
    width, half = wd0.shape[0], low_ref.shape[0]
    left, right = pl.ds(0, width), pl.ds(width, width)
    total = plain(hidden_ref[:, left], wd0[...]) + plain(hidden_ref[:, right], wd1[...])
    low_ref[...] = total[:half].astype(bf16)
    high_ref[...] = total[half:].astype(bf16)


def side_kernel(y_ref, hidden_ref, wd0, wd1, *refs):
    out_refs, rows = refs[:3], refs[3]
    width = wd0.shape[0]
    left, right = pl.ds(0, width), pl.ds(width, width)
    rows[...] = (
        plain(hidden_ref[:, left], wd0[...]) + plain(hidden_ref[:, right], wd1[...])
    ).astype(bf16)

    for k, ref in enumerate(out_refs):

        @pl.when(pl.program_id(0) == k)
        def _(ref=ref):
            ref[...] = rows[...]


def back_kernel(y_ref, *refs):
    u_refs, (wd0, wd1, out_ref, rows) = refs[:5], refs[5:]
    width = wd0.shape[0]
    left, right = pl.ds(0, width), pl.ds(width, width)
    step = pl.program_id(0)

    @pl.when(step == 0)
    def _():
        out_ref[...] = jnp.zeros_like(out_ref)

    load_piece(step, u_refs, rows)
    out_ref[:, left] += cross(rows[...], wd0[...])
    out_ref[:, right] += cross(rows[...], wd1[...])


def bwd_kernel(y_ref, *refs):
    wg0, wg1, wu0, wu1, rh_ref, meta_ref, seq_ref, partial_ref, slope_ref, silu_ref = refs[:10]
    gate_grad_ref, up_grad_ref, coef_ref, low_ref, high_ref = refs[10:15]
    width, half = wg0.shape[0], low_ref.shape[0]
    left, right = pl.ds(0, width), pl.ds(width, width)
    count = partial_ref.shape[0]
    blocks = seq_ref.shape[0]
    lane = lax.broadcasted_iota(jnp.int32, (blocks, 128), 1)
    first = jnp.broadcast_to(seq_ref[:, pl.ds(0, 1)], lane.shape)
    second = jnp.broadcast_to(seq_ref[:, pl.ds(1, 1)], lane.shape)
    by_lane = jnp.where(lane < 2, first, jnp.where(lane < 4, second, 0.0))
    shares = meta_ref[...].astype(f32).reshape(blocks, count // blocks, 128)
    terms = (shares * by_lane[:, None, :]).reshape(count, 128)
    coef_ref[...] = jnp.sum(terms, axis=1, keepdims=True)
    chunk = count // 8

    @pl.loop(0, 8)
    def _(i):
        at = pl.ds(pl.multiple_of(i * chunk, chunk), chunk)
        hidden_grad = partial_ref[at] + coef_ref[at] * rh_ref[...]
        gate_grad_ref[at] = (hidden_grad * slope_ref[at]).astype(bf16)
        up_grad_ref[at] = (hidden_grad * silu_ref[at]).astype(bf16)

    total = (
        plain(gate_grad_ref[:, left], wg0[...])
        + plain(gate_grad_ref[:, right], wg1[...])
        + plain(up_grad_ref[:, left], wu0[...])
        + plain(up_grad_ref[:, right], wu1[...])
    )
    low_ref[...] = total[:half].astype(bf16)
    high_ref[...] = total[half:].astype(bf16)


def rest_kernel(y_ref, *refs):
    wg0, wg1, wu0, wu1, gate_grad_ref, up_grad_ref = refs[:6]
    out_refs, rows = refs[6:9], refs[9]
    width = wg0.shape[0]
    left, right = pl.ds(0, width), pl.ds(width, width)
    rows[...] = (
        plain(gate_grad_ref[:, left], wg0[...])
        + plain(gate_grad_ref[:, right], wg1[...])
        + plain(up_grad_ref[:, left], wu0[...])
        + plain(up_grad_ref[:, right], wu1[...])
    ).astype(bf16)

    for k, ref in enumerate(out_refs):

        @pl.when(pl.program_id(0) == k)
        def _(ref=ref):
            ref[...] = rows[...]


def grad_kernel(y_ref, *refs):
    x_refs, u_refs = refs[:5], refs[5:10]
    hidden_ref, gate_grad_ref, up_grad_ref, coef_ref, rh_ref = refs[10:15]
    own_ref, other_ref, left, rows = refs[15:]
    width = left.shape[1]
    step = pl.program_id(0)

    @pl.when(step == 0)
    def _():
        for i, ref in enumerate((gate_grad_ref, up_grad_ref, hidden_ref)):
            turned = ref[...].T
            left[2 * i] = turned[:width]
            left[2 * i + 1] = turned[width:]

    load_piece(step, x_refs, rows.at[0])
    load_piece(step, u_refs, rows.at[1])
    rows[1] = (rows[1].astype(f32) + coef_ref[...] * rh_ref[...]).astype(bf16)

    @pl.loop(0, 3)
    def _(i):
        at = pl.ds(pl.multiple_of(i * width, width), width)
        own_ref[at] = plain(left[2 * i], rows[i // 2]).astype(bf16)
        other_ref[at] = plain(left[2 * i + 1], rows[i // 2]).astype(bf16)


def whole(shape):
    return pl.BlockSpec(shape, lambda k, y: (0,) * len(shape))


def columns(width, block):
    return pl.BlockSpec((width, block), lambda k, y: (0, (y[0] + k) % 4))


def near_columns(width, block):
    return pl.BlockSpec((width, block), lambda k, y: (0, (y[0] + k + k // 2) % 4))


def far_columns(width, block):
    return pl.BlockSpec((width, block), lambda k, y: (0, (y[0] + 2) % 4))


def piece_specs(rows, block):
    full, part = whole((rows, block)), whole((rows // 2, block))
    return [full, full, part, part, full]


def call(kernel, steps, in_specs, out_specs, out_shape, scratch, flops, args):
    return pl.pallas_call(
        kernel,
        grid_spec=pltpu.PrefetchScalarGridSpec(
            num_scalar_prefetch=1,
            grid=(steps,),
            in_specs=in_specs,
            out_specs=out_specs,
            scratch_shapes=scratch,
        ),
        out_shape=out_shape,
        compiler_params=pltpu.CompilerParams(
            dimension_semantics=("arbitrary",), vmem_limit_bytes=VMEM_MIB * 1024 * 1024
        ),
        cost_estimate=pl.CostEstimate(flops=flops, bytes_accessed=20_000_000, transcendentals=0),
    )(*args)


def layer(
    tokens, expert_ids, route_share, w_gate, w_up, w_down, reward_head, upstream, pair_order
):
    tok_count, local_width = tokens.shape
    capacity = tok_count * expert_ids.shape[1] // EXPERTS
    ep_size = lax.axis_size(EP)
    replicas = ep_size // EXPERTS
    half_cap = capacity // 2
    block = 2 * local_width
    rows = ep_size * half_cap
    hid = w_gate.shape[0]
    core = lax.axis_index("tp_c")
    place = jnp.stack([lax.axis_index("tp_y"), core]).astype(jnp.int32)

    wg_other, wu_other, wd_other = swap(w_gate), swap(w_up), swap(w_down)

    seq_local = tok_count // SEQ_LEN
    half_slots = EXPERTS * half_cap
    half_rows = jax.ShapeDtypeStruct((half_slots, block), bf16)
    mine, theirs, meta, picker, mixing = call(
        route_kernel,
        1,
        [whole((2, tok_count)), whole((1, tok_count))] + [whole((tok_count, local_width))] * 2,
        [whole((half_slots, block))] * 2
        + [whole((half_slots, 128))]
        + [whole((2 * half_slots, tok_count))] * 2,
        [
            half_rows,
            half_rows,
            jax.ShapeDtypeStruct((half_slots, 128), bf16),
            jax.ShapeDtypeStruct((2 * half_slots, tok_count), bf16),
            jax.ShapeDtypeStruct((2 * half_slots, tok_count), f32),
        ],
        [
            pltpu.VMEM((2 * half_slots, block), bf16),
            pltpu.VMEM((2 * half_slots, 128), bf16),
        ],
        1_000_000,
        (place, expert_ids.T, route_share[None, :], tokens, upstream),
    )
    theirs = swap(theirs)
    half_spec = whole((half_slots, block))
    token_block = call(
        pack_kernel,
        1,
        [half_spec] * 2,
        whole((rows, block)),
        jax.ShapeDtypeStruct((rows, block), bf16),
        [],
        1_000_000,
        (place, mine, theirs),
    )
    grad_block = call(
        pack_kernel,
        1,
        [half_spec] * 2 + [whole((half_slots, 128))],
        whole((rows, block + 128)),
        jax.ShapeDtypeStruct((rows, block + 128), bf16),
        [],
        1_000_000,
        (place, mine, theirs, meta),
    )

    def to_experts(block_rows):
        width = block_rows.shape[1]
        return exchange(block_rows.reshape(ep_size, half_cap, width)).reshape(rows, width)

    token_rows = to_experts(token_block)
    grad_full = to_experts(grad_block)

    head = lax.all_gather(reward_head, TP, axis=0, tiled=True)
    head_own = jnp.sum(w_down.astype(f32) * head[None, :], axis=1)
    head_other = jnp.sum(wd_other.astype(f32) * head[None, :], axis=1)
    head_row = jnp.concatenate([head_own, head_other])[None, :]
    local_scores = jnp.sum(tokens.astype(f32) * reward_head[None, :], axis=1)
    local_rewards = jnp.sum(local_scores.reshape(seq_local, SEQ_LEN), axis=1)
    seq_total = pair_order.shape[0]
    offset = lax.axis_index(EP) * seq_local
    placed = lax.dynamic_update_slice(jnp.zeros((seq_total,), f32), local_rewards, (offset,))
    token_rows, head_row, placed = lax.optimization_barrier((token_rows, head_row, placed))

    token_pieces = gather_features(token_rows)
    grad_pieces = gather_features(grad_full[:, :block])

    slots_hid = (rows, 2 * hid)
    meta_spec = pl.BlockSpec((rows, 128), lambda k, y: (0, block // 128))
    work = rows * 2 * hid * 4 * block
    own_rows, ahead_rows, far_low, far_high, back_rows = token_pieces
    gate_weights = (w_gate, wg_other, w_up, wu_other)
    full, part = whole((rows, block)), whole((rows // 2, block))
    gate, up = call(
        near_kernel,
        3,
        [full] * 3 + [near_columns(hid, block)] * 4,
        [whole(slots_hid)] * 2,
        [jax.ShapeDtypeStruct(slots_hid, f32)] * 2,
        [pltpu.VMEM((rows, block), bf16)],
        3 * work,
        (place, own_rows, ahead_rows, back_rows, *gate_weights),
    )
    slope, silu, hidden, score = call(
        fwd_kernel,
        1,
        [part] * 2
        + [far_columns(hid, block)] * 4
        + [whole((1, 2 * hid)), meta_spec]
        + [whole(slots_hid)] * 2,
        [whole(slots_hid)] * 3 + [whole((ep_size, 128))],
        [jax.ShapeDtypeStruct(slots_hid, f32)] * 2
        + [jax.ShapeDtypeStruct(slots_hid, bf16), jax.ShapeDtypeStruct((ep_size, 128), f32)],
        [pltpu.VMEM(slots_hid, f32)] * 2 + [pltpu.VMEM((rows, block), bf16)],
        work,
        (place, far_low, far_high, *gate_weights, head_row, grad_full, gate, up),
    )
    placed = (placed + score[:, :seq_local].reshape(seq_total)).reshape(2, 1, seq_total // 2)
    everyone = lax.axis_size(EP_TP)
    spread = jnp.broadcast_to(placed, (2, everyone, seq_total // 2))
    spread = lax.all_to_all(spread, EP_TP, split_axis=1, concat_axis=1, tiled=True)
    rewards = jnp.sum(spread, axis=1).reshape(seq_total) / math.sqrt(SEQ_LEN)

    half_shape = jax.ShapeDtypeStruct((rows // 2, block), bf16)
    full_shape = jax.ShapeDtypeStruct((rows, block), bf16)
    down_low, down_high = call(
        down_kernel,
        1,
        [whole(slots_hid)] + [far_columns(hid, block)] * 2,
        [part] * 2,
        [half_shape] * 2,
        [],
        work // 2,
        (place, hidden, w_down, wd_other),
    )
    down_own, down_ahead, down_back = call(
        side_kernel,
        3,
        [whole(slots_hid)] + [near_columns(hid, block)] * 2,
        [full] * 3,
        [full_shape] * 3,
        [pltpu.VMEM((rows, block), bf16)],
        3 * work // 2,
        (place, hidden, w_down, wd_other),
    )
    down_pieces = (down_own, down_ahead, down_low, down_high, down_back)
    partial = call(
        back_kernel,
        4,
        piece_specs(rows, block) + [columns(hid, block)] * 2,
        [whole(slots_hid)],
        [jax.ShapeDtypeStruct(slots_hid, f32)],
        [pltpu.VMEM((rows, block), bf16)],
        2 * work,
        (place, *grad_pieces, w_down, wd_other),
    )[0]
    down_sums = scatter_start(down_pieces)

    seq_iota = jnp.arange(seq_total, dtype=jnp.int32)
    chosen_hot = (pair_order[0::2][:, None] == seq_iota[None, :]).astype(f32)
    rejected_hot = (pair_order[1::2][:, None] == seq_iota[None, :]).astype(f32)
    margin = jnp.sum((chosen_hot - rejected_hot) * rewards[None, :], axis=1)
    pair_loss = jnp.mean(jax.nn.softplus(-margin))
    pair_weight = jax.nn.sigmoid(-margin)
    seq_coef = jnp.sum(pair_weight[:, None] * (rejected_hot - chosen_hot), axis=0)
    token_coef = jnp.repeat(lax.dynamic_slice_in_dim(seq_coef, offset, seq_local), SEQ_LEN)
    grad_out = (
        upstream.astype(f32)
        + loss_scale * token_coef[:, None] * reward_head[None, :] / math.sqrt(SEQ_LEN)
    ).astype(bf16)
    scaled = (seq_coef * (loss_scale / math.sqrt(SEQ_LEN))).reshape(ep_size, seq_local)

    gate_grad, up_grad, slot_coef, far_low, far_high = call(
        bwd_kernel,
        1,
        [far_columns(hid, block)] * 4
        + [whole((1, 2 * hid)), meta_spec, whole((ep_size, seq_local))]
        + [whole(slots_hid)] * 3,
        [whole(slots_hid)] * 2 + [whole((rows, 1))] + [part] * 2,
        [jax.ShapeDtypeStruct(slots_hid, bf16)] * 2
        + [jax.ShapeDtypeStruct((rows, 1), f32)]
        + [jax.ShapeDtypeStruct((rows // 2, block), bf16)] * 2,
        [],
        work,
        (place, *gate_weights, head_row, grad_full, scaled, partial, slope, silu),
    )
    own_sums, ahead_sums, back_sums = call(
        rest_kernel,
        3,
        [near_columns(hid, block)] * 4 + [whole(slots_hid)] * 2,
        [full] * 3,
        [jax.ShapeDtypeStruct((rows, block), bf16)] * 3,
        [pltpu.VMEM((rows, block), bf16)],
        3 * work,
        (place, *gate_weights, gate_grad, up_grad),
    )
    input_sums = scatter_start((own_sums, ahead_sums, far_low, far_high, back_sums))

    own_grads, other_grads = call(
        grad_kernel,
        4,
        piece_specs(rows, block) * 2
        + [whole(slots_hid)] * 3
        + [whole((rows, 1)), columns(1, block)],
        [columns(3 * hid, block)] * 2,
        [jax.ShapeDtypeStruct((3 * hid, 4 * block), bf16)] * 2,
        [pltpu.VMEM((6, hid, rows), bf16), pltpu.VMEM((2, rows, block), bf16)],
        6 * work,
        (place, *token_pieces, *grad_pieces, hidden, gate_grad, up_grad, slot_coef, head[None, :]),
    )
    other_grads = swap(other_grads)
    grad_gate, grad_up, grad_down = (
        add(own_grads[i * hid : (i + 1) * hid], other_grads[i * hid : (i + 1) * hid])
        for i in range(3)
    )

    def come_back(pieces):
        summed = add(*pieces).reshape(ep_size, half_cap, block)
        arrived = exchange(summed).astype(f32)
        sums = jnp.sum(arrived.reshape(EXPERTS, replicas, half_cap, block), axis=1)
        sums = sums.astype(bf16).reshape(EXPERTS * half_cap, block)
        left, right = sums[:, :local_width], sums[:, local_width:]
        mine = jnp.where(core == 0, left, right)
        theirs = swap(jnp.where(core == 0, right, left))
        return jnp.concatenate(
            [jnp.where(core == 0, mine, theirs), jnp.where(core == 0, theirs, mine)], axis=0
        )

    mixed_sum = across(mixing, come_back(down_sums).astype(f32))
    layer_out = (tokens.astype(f32) + mixed_sum).astype(bf16)
    returned = across(picker, come_back(input_sums))
    grad_tokens = (grad_out.astype(f32) + returned).astype(bf16)
    return (layer_out, rewards, pair_loss, grad_tokens, grad_gate, grad_up, grad_down)


def solution(mesh):
    split = Mesh(mesh.devices.reshape(4, 8, 4, 2), EP_TP)
    in_specs = (
        P(EP, TP),
        P(EP, None),
        P(EP),
        P(EP_TP, None),
        P(EP_TP, None),
        P(EP_TP, None),
        P(TP),
        P(EP, TP),
        P(),
    )
    out_specs = (P(EP, TP), P(), P(), P(EP, TP), P(EP_TP, None), P(EP_TP, None), P(EP_TP, None))
    return jax.shard_map(layer, mesh=split, in_specs=in_specs, out_specs=out_specs, check_vma=False)
```
